32 devices in a mesh: ctx: 8 (over z, x), tp: 4 (over y, core).
Axes of the slice: x: 2, y: 2, z: 4, core: 2. Of those that a mesh axis runs over, the one named last changes fastest.
Arguments:
- queries: bfloat16 [2048, 8192], P('ctx', 'tp'), may hold values from -8 to 8
- keys: bfloat16 [2048, 1024], P('ctx'), may hold values from -7 to 7
- values: bfloat16 [2048, 1024], P('ctx'), may hold values from -6 to 6
- out_weight: bfloat16 [8192, 4096], P('tp'), may hold values from -0.25 to 0.25
- block_order: int32 [16], P('ctx'), may hold values from 0 to 15, each once
Outputs:
- projected: bfloat16 [2048, 4096], P('ctx', 'tp')
The draws below stay inside these ranges and needn't reach their ends.
Inputs may be any that keep to these rules, and one draw needn't show every extreme that they name: `block_order`: every sequence block appears exactly once.
All inputs are finite; a program needn't handle non-finite values.
Results may differ from the reference program's by a relative error of at most 0.015.
Values may be sent and summed in bfloat16 or wider, within the bound.
No kernel may reach another device: no remote copies, remote signals or barrier semaphores. Data moves between devices by JAX's collectives and lax.ppermute only.
A program may use at most 64 MiB of HBM per device.

```python
import math
import jax
import jax.numpy as jnp
from jax import lax

QUERY_HEADS = 64
KEY_VALUE_HEADS = 8
HEAD_SIZE = 128
DW = 4096
BLK = 128
SEQUENCE_TOKENS = 2048
NBLK = 16


def shared_vectors(key):
    key_random_keys = jax.random.fold_in(key, 11)
    key_queries = jax.random.fold_in(key, 12)
    key_collection = jnp.clip(jax.random.normal(key_random_keys, (SEQUENCE_TOKENS, KEY_VALUE_HEADS * HEAD_SIZE), jnp.float32), -6.0, 6.0)
    queryset = jnp.clip(2.5 * jax.random.normal(key_queries, (SEQUENCE_TOKENS, QUERY_HEADS * HEAD_SIZE), jnp.float32), -8.0, 8.0)
    return (key_collection.astype(jnp.bfloat16), queryset.astype(jnp.bfloat16))


def draw_queries(key, part):
    return shared_vectors(key)[1]


def draw_keys(key, part):
    return shared_vectors(key)[0]


def steps_of(key, shape, split, least, largest):
    def one(dim, parts):
        heights = jax.random.uniform(jax.random.fold_in(jax.random.fold_in(key, 6), dim), (parts,), jnp.float32, least / len(split), largest / len(split))
        return jnp.repeat(jnp.exp(heights), shape[dim] // parts).reshape((-1,) + (1,) * (len(shape) - dim - 1))

    gain = one(*split[0])
    for cut in split[1:]:
        gain = gain * one(*cut)
    return gain


def noise(key, extent, deviation, bound, cuts=(), kind=jnp.bfloat16):
    drawn = jax.random.normal(key, extent, jnp.float32) * deviation
    if len(cuts) > 0:
        drawn = steps_of(key, extent, cuts, -0.22, 0.18) * drawn
    return jnp.clip(drawn, min=-bound, max=bound).astype(kind)


def setup_inputs(seed: int = 0) -> dict:
    key_list = jax.random.split(jax.random.key(seed), 6)
    return {
        "queries": draw_queries(jax.random.fold_in(key_list[5], 71), 0),
        "keys": draw_keys(jax.random.fold_in(key_list[5], 71), 0),
        "values": noise(key_list[2], (SEQUENCE_TOKENS, KEY_VALUE_HEADS * HEAD_SIZE), 1.0, 6.0, ((0, 8),)),
        "out_weight": noise(key_list[3], (QUERY_HEADS * HEAD_SIZE, DW), (QUERY_HEADS * HEAD_SIZE // 16) ** -0.5, 0.25, ((0, 4),)),
        "block_order": jax.random.permutation(key_list[4], NBLK).astype(jnp.int32),
    }


def reference(queries, keys, values, out_weight, block_order):
    head_group = QUERY_HEADS // KEY_VALUE_HEADS
    offsets = jnp.arange(BLK, dtype=jnp.int32)
    positions = (block_order[:, None].astype(jnp.int32) * BLK + offsets[None, :]).reshape(-1)
    scale = 1.0 / math.sqrt(HEAD_SIZE)
    q_heads = jnp.transpose(queries.reshape(SEQUENCE_TOKENS, QUERY_HEADS, HEAD_SIZE), (1, 0, 2))
    key_head_rows = jnp.transpose(keys.reshape(SEQUENCE_TOKENS, KEY_VALUE_HEADS, HEAD_SIZE), (1, 0, 2))
    value_head_rows = jnp.transpose(values.reshape(SEQUENCE_TOKENS, KEY_VALUE_HEADS, HEAD_SIZE), (1, 0, 2))
    q_pos = positions.reshape(SEQUENCE_TOKENS // BLK, BLK)

    def one_head(head):
        k_rows = key_head_rows[head // head_group]
        v_rows = value_head_rows[head // head_group]
        q_blocks = q_heads[head].reshape(SEQUENCE_TOKENS // BLK, BLK, HEAD_SIZE)

        def one_block(item):
            q_rows, rows_pos = item
            scores = jnp.dot(q_rows, k_rows.T, preferred_element_type=jnp.float32) * scale
            visible = positions[None, :] <= rows_pos[:, None]
            top = lax.optimization_barrier(jnp.max(jnp.where(visible, scores, -jnp.inf), axis=1, keepdims=True))
            weights = jnp.where(visible, jnp.exp(scores - top), 0.0)
            total = lax.optimization_barrier(jnp.sum(weights, axis=1, keepdims=True))
            return jnp.dot(weights.astype(jnp.bfloat16), v_rows, preferred_element_type=jnp.float32) / total
        return lax.map(one_block, (q_blocks, q_pos)).reshape(SEQUENCE_TOKENS, HEAD_SIZE)
    heads_out = lax.map(one_head, jnp.arange(QUERY_HEADS, dtype=jnp.int32))
    attended = jnp.transpose(heads_out, (1, 0, 2)).reshape(SEQUENCE_TOKENS, QUERY_HEADS * HEAD_SIZE).astype(jnp.bfloat16)
    return jnp.dot(attended, out_weight, preferred_element_type=jnp.float32).astype(jnp.bfloat16)
```

```python
import functools
import math

import jax
import jax.numpy as jnp
from jax import lax
from jax.experimental import pallas as pl
from jax.experimental.pallas import tpu as pltpu
from jax.sharding import PartitionSpec as P

QUERY_HEADS = 64
KEY_VALUE_HEADS = 8
HEAD_SIZE = 128
HIDDEN = -1e30
TAIL = 16


def attend_kernel(n_blocks, first, last, scale, *refs):
    order_ref, q_ref = refs[:2]
    blocks = refs[2 : 2 + n_blocks]
    refs = refs[2 + n_blocks :]
    if not first:
        old_m, old_l, old_acc = refs[:3]
        refs = refs[3:]
    outs = refs[: 1 if last else 3]
    stacked = refs[-1]
    rows = q_ref.shape[0]
    heads = q_ref.shape[1] // HEAD_SIZE
    span = 2 * rows if heads % 2 == 0 else rows
    own = order_ref[pl.program_id(1)]

    for head in range(heads):
        stacked[head * rows : (head + 1) * rows, :] = q_ref[
            :, head * HEAD_SIZE : (head + 1) * HEAD_SIZE
        ]
    key_at = lax.broadcasted_iota(jnp.int32, (rows, rows), 0)
    query_at = lax.broadcasted_iota(jnp.int32, (rows, rows), 1) + own * rows
    query_at = query_at.astype(jnp.float32)
    key_at = key_at.astype(jnp.float32)
    keys, values, bias = [], [], []
    for block in blocks:
        length = block.shape[0] - TAIL
        keys.append(block[0:length, 0:HEAD_SIZE])
        values.append(block[0:length, HEAD_SIZE : 2 * HEAD_SIZE])
        tail = block[length : length + TAIL, 0:HEAD_SIZE].astype(jnp.float32)
        tiles = []
        for part in range(length // rows):
            number = tail[2 * part : 2 * part + 1, :] * 128.0 + tail[2 * part + 1 : 2 * part + 2, :]
            hidden = number[:, 0:rows] * float(rows) + key_at > query_at
            tiles.append(jnp.where(hidden, HIDDEN, 0.0))
        tile = jnp.concatenate(tiles, axis=0)
        bias.append(jnp.concatenate([tile] * (span // rows), axis=1))

    for piece in range(heads * rows // span):
        at = slice(piece * span, (piece + 1) * span)
        q = stacked[at, :]
        scores = []
        for key, tile in zip(keys, bias):
            score = lax.dot_general(
                key, q, (((1,), (1,)), ((), ())), preferred_element_type=jnp.float32
            )
            scores.append(score * scale + tile)
        top = jnp.max(scores[0], axis=0, keepdims=True)
        for score in scores[1:]:
            top = jnp.maximum(top, jnp.max(score, axis=0, keepdims=True))
        if not first:
            top = jnp.maximum(top, old_m[0, :, at])
        total = None
        acc = None
        for score, value in zip(scores, values):
            weight = jnp.exp2(score - top)
            part = jnp.sum(weight, axis=0, keepdims=True)
            spread = lax.dot_general(
                value,
                weight.astype(jnp.bfloat16),
                (((0,), (0,)), ((), ())),
                preferred_element_type=jnp.float32,
            )
            total = part if total is None else total + part
            acc = spread if acc is None else acc + spread
        if not first:
            factor = jnp.exp2(old_m[0, :, at] - top)
            total = total + old_l[0, :, at] * factor
            acc = acc + old_acc[0, :, at] * factor
        if last:
            done = (acc / total).T.astype(jnp.bfloat16)
            for k in range(span // rows):
                head = piece * (span // rows) + k
                outs[0][:, head * HEAD_SIZE : (head + 1) * HEAD_SIZE] = done[
                    k * rows : (k + 1) * rows, :
                ]
        else:
            outs[0][0, :, at] = top
            outs[1][0, :, at] = total
            outs[2][0, :, at] = acc


def attend(order, queries, blocks, state, last, kv_heads):
    tokens, width = queries.shape
    parts = order.shape[0]
    rows = tokens // parts
    group = width // kv_heads
    lanes = group // HEAD_SIZE * rows
    scale = math.log2(math.e) / math.sqrt(HEAD_SIZE)
    first = state is None
    state_spec = [
        pl.BlockSpec((1, 1, lanes), lambda k, i: (k * parts + i, 0, 0)),
        pl.BlockSpec((1, 1, lanes), lambda k, i: (k * parts + i, 0, 0)),
        pl.BlockSpec((1, HEAD_SIZE, lanes), lambda k, i: (k * parts + i, 0, 0)),
    ]
    state_shape = [
        jax.ShapeDtypeStruct((kv_heads * parts, 1, lanes), jnp.float32),
        jax.ShapeDtypeStruct((kv_heads * parts, 1, lanes), jnp.float32),
        jax.ShapeDtypeStruct((kv_heads * parts, HEAD_SIZE, lanes), jnp.float32),
    ]
    q_spec = pl.BlockSpec((rows, group), lambda k, i: (i, k))
    in_specs = [pl.BlockSpec(memory_space=pltpu.SMEM), q_spec]
    for block in blocks:
        in_specs.append(pl.BlockSpec((block.shape[0], 2 * HEAD_SIZE), lambda k, i: (0, k)))
    if not first:
        in_specs += state_spec
    pairs = tokens * width // HEAD_SIZE * sum(b.shape[0] - TAIL for b in blocks)
    return pl.pallas_call(
        functools.partial(attend_kernel, len(blocks), first, last, scale),
        grid=(kv_heads, parts),
        in_specs=in_specs,
        out_specs=[q_spec] if last else state_spec,
        out_shape=[jax.ShapeDtypeStruct(queries.shape, jnp.bfloat16)] if last else state_shape,
        scratch_shapes=[pltpu.VMEM((lanes, HEAD_SIZE), jnp.bfloat16)],
        cost_estimate=pl.CostEstimate(
            flops=4 * pairs * HEAD_SIZE, bytes_accessed=4 * pairs, transcendentals=pairs
        ),
    )(order, queries, *blocks, *(() if first else state))


def project_kernel(tiles, at_ref, a_ref, w_ref, send_ref, keep_ref):
    step = pl.program_id(0)
    product = jnp.dot(a_ref[...], w_ref[...], preferred_element_type=jnp.float32)

    @pl.when(step < tiles)
    def _():
        send_ref[...] = product.astype(jnp.bfloat16)

    @pl.when(step >= tiles)
    def _():
        keep_ref[...] = product


def project(attended, weight, send_at, keep_at, columns):
    tokens, depth = attended.shape
    wide = math.gcd(columns, 256)
    tiles = columns // wide
    at = jnp.stack([send_at // wide, keep_at // wide]).astype(jnp.int32)
    return pl.pallas_call(
        functools.partial(project_kernel, tiles),
        grid_spec=pltpu.PrefetchScalarGridSpec(
            num_scalar_prefetch=1,
            grid=(2 * tiles,),
            in_specs=[
                pl.BlockSpec((tokens, depth), lambda s, at: (0, 0)),
                pl.BlockSpec(
                    (depth, wide),
                    lambda s, at: (0, jnp.where(s < tiles, at[0] + s, at[1] + s - tiles)),
                ),
            ],
            out_specs=[
                pl.BlockSpec((tokens, wide), lambda s, at: (0, jnp.minimum(s, tiles - 1))),
                pl.BlockSpec((tokens, wide), lambda s, at: (0, jnp.maximum(s - tiles, 0))),
            ],
        ),
        out_shape=[
            jax.ShapeDtypeStruct((tokens, columns), jnp.bfloat16),
            jax.ShapeDtypeStruct((tokens, columns), jnp.float32),
        ],
        cost_estimate=pl.CostEstimate(
            flops=4 * tokens * depth * columns,
            bytes_accessed=4 * depth * columns,
            transcendentals=0,
        ),
    )(at, attended, weight)


def shards(n_ctx, n_tp, queries, keys, values, out_weight, block_order):
    tokens = queries.shape[0]
    heads_dev = queries.shape[1] // HEAD_SIZE
    group_size = QUERY_HEADS // KEY_VALUE_HEADS
    kv_heads = max(1, heads_dev // group_size)
    tp = lax.axis_index("tp")
    start = tp * heads_dev // group_size * HEAD_SIZE
    own_keys = lax.dynamic_slice_in_dim(keys, start, kv_heads * HEAD_SIZE, 1)
    own_values = lax.dynamic_slice_in_dim(values, start, kv_heads * HEAD_SIZE, 1)
    pieces = []
    for head in range(kv_heads):
        at = slice(head * HEAD_SIZE, (head + 1) * HEAD_SIZE)
        pieces += [own_keys[:, at], own_values[:, at]]
    body = jnp.concatenate(pieces, axis=1)
    digits = jnp.stack([block_order // 128, block_order % 128], axis=1).reshape(-1)
    digits = jnp.pad(digits, (0, TAIL - digits.shape[0])).astype(jnp.bfloat16)
    tail = jnp.broadcast_to(digits[:, None], (TAIL, body.shape[1]))
    own = jnp.concatenate([body, tail], axis=0)

    inner = math.gcd(n_ctx, 2)
    outer = n_ctx // inner

    def along_outer(block, k):
        pairs = [
            (o * inner + i, (o + k) % outer * inner + i) for o in range(outer) for i in range(inner)
        ]
        return lax.ppermute(block, "ctx", pairs)

    def along_inner(block, k):
        pairs = [
            (o * inner + i, o * inner + (i + k) % inner) for o in range(outer) for i in range(inner)
        ]
        return lax.ppermute(block, "ctx", pairs)

    shifts = []
    for k in range(1, outer // 2 + 1):
        shifts += [k] if 2 * k == outer else [k, outer - k]
    column = [own] + [along_outer(own, k) for k in shifts]
    crossed = [[along_inner(block, k) for k in range(1, inner)] for block in column]
    arrived = []
    for block, others in zip(column, crossed):
        arrived += [block] + others

    stages = [arrived[i : i + 3] for i in range(0, len(arrived) - 2, 3)]
    seen = sum(len(s) for s in stages)
    stages += [[b] for b in arrived[seen:]]
    state = None
    for index, blocks in enumerate(stages):
        state = attend(
            block_order, queries, blocks, state, index == len(stages) - 1, kv_heads
        )
    attended = state[0]

    columns = out_weight.shape[1] // n_tp
    cores = math.gcd(n_tp, 2)
    groups = n_tp // cores
    core, grp = tp % cores, tp // cores

    def to_core(x):
        pairs = [(t, t // cores * cores + (t + 1) % cores) for t in range(n_tp)]
        return lax.ppermute(x, "tp", pairs)

    def to_group(x, r):
        pairs = [(t, (t + r * cores) % n_tp) for t in range(n_tp)]
        return lax.ppermute(x, "tp", pairs)

    def summed_on_chip(r, at, width):
        to = (grp + r) % groups * cores
        send, keep = project(
            attended,
            out_weight,
            (to + (core + 1) % cores) * columns + at,
            (to + core) * columns + at,
            width,
        )
        if cores == 1:
            return keep
        return keep + to_core(send).astype(jnp.float32)

    cuts = 2 if groups == 2 else 1
    width = columns // cuts
    arriving = []
    for cut in range(cuts):
        arriving.append(
            [
                to_group(summed_on_chip(r, cut * width, width).astype(jnp.bfloat16), r)
                for r in range(1, groups)
            ]
        )
    mine = summed_on_chip(0, 0, columns)
    result = []
    for cut in range(cuts):
        total = mine[:, cut * width : (cut + 1) * width]
        for x in arriving[cut]:
            total = total + x.astype(jnp.float32)
        result.append(total.astype(jnp.bfloat16))
    return jnp.concatenate(result, axis=1)


def solution(mesh):
    in_specs = (P("ctx", "tp"), P("ctx", None), P("ctx", None), P("tp", None), P("ctx"))
    out_specs = P("ctx", "tp")
    body = functools.partial(shards, mesh.shape["ctx"], mesh.shape["tp"])
    return jax.shard_map(body, mesh=mesh, in_specs=in_specs, out_specs=out_specs, check_vma=False)
```

```python
import functools
import math

import jax
import jax.numpy as jnp
from jax import lax
from jax.experimental import pallas as pl
from jax.experimental.pallas import tpu as pltpu
from jax.sharding import PartitionSpec as P

QUERY_HEADS = 64
KEY_VALUE_HEADS = 8
HEAD_SIZE = 128
HIDDEN = -1e30
TAIL = 16
DIGIT = 128
NT = (((1,), (1,)), ((), ()))
VMEM_LIMIT = 16 << 20


def attend_kernel(n_blocks, first, last, scale, kv_heads, span, *refs):
    order_ref, q_ref = refs[:2]
    blocks = refs[2 : 2 + n_blocks]
    refs = refs[2 + n_blocks :]
    if not first:
        old_top, old_total, old_acc = refs[:3]
        refs = refs[3:]
    outs = refs[: 1 if last else 3]
    bias_ref, flip_ref = refs[-6:-4]
    score_refs, weight_refs = refs[-4:-2], refs[-2:]
    parts = order_ref.shape[0]
    rows = q_ref.shape[0] // parts
    heads = q_ref.shape[1] // kv_heads // HEAD_SIZE
    pair = span // rows
    lengths = [block.shape[0] - TAIL for block in blocks]
    offsets = [sum(lengths[:b]) for b in range(n_blocks)]

    key_at = lax.broadcasted_iota(jnp.int32, (rows, rows), 0).astype(jnp.float32)
    query_iota = lax.broadcasted_iota(jnp.int32, (rows, rows), 1)
    for block, length, offset in zip(blocks, lengths, offsets):
        tail = block[length : length + TAIL, 0:HEAD_SIZE].astype(jnp.float32)
        for part in range(length // rows):
            high, low = tail[2 * part : 2 * part + 1, :], tail[2 * part + 1 : 2 * part + 2, :]
            key_pos = (high * DIGIT + low)[:, 0:rows] * float(rows) + key_at
            at = slice(offset + part * rows, offset + (part + 1) * rows)
            for i in range(parts):
                query_pos = (query_iota + order_ref[i] * rows).astype(jnp.float32)
                bias_ref[i, at, :] = jnp.where(key_pos > query_pos, HIDDEN, 0.0)
        for k in range(kv_heads):
            at = slice((2 * k + 1) * HEAD_SIZE, (2 * k + 2) * HEAD_SIZE)
            flip_ref[k, :, offset : offset + length] = block[0:length, at].T

    pieces = [
        (k, i, p) for k in range(kv_heads) for i in range(parts) for p in range(heads // pair)
    ]
    tops, totals = {}, {}

    def head_cols(k, p, j):
        head = k * heads + p * pair + j
        return slice(head * HEAD_SIZE, (head + 1) * HEAD_SIZE)

    def score(t):
        k, i, p = pieces[t]
        q = jnp.concatenate(
            [q_ref[i * rows : (i + 1) * rows, head_cols(k, p, j)] for j in range(pair)], axis=0
        )
        top = None
        for block, length, offset in zip(blocks, lengths, offsets):
            key = block[0:length, 2 * k * HEAD_SIZE : (2 * k + 1) * HEAD_SIZE]
            tile = bias_ref[i, offset : offset + length, :]
            scores = lax.dot_general(key, q, NT, preferred_element_type=jnp.float32)
            scores = scores * scale + jnp.concatenate([tile] * pair, axis=1)
            score_refs[t % 2][offset : offset + length, :] = scores
            part = jnp.max(scores, axis=0, keepdims=True)
            top = part if top is None else jnp.maximum(top, part)
        if not first:
            top = jnp.maximum(top, old_top[k * parts + i, :, p * span : (p + 1) * span])
        tops[t] = top

    def weigh(t):
        weights = jnp.exp2(score_refs[t % 2][...] - tops[t])
        totals[t] = jnp.sum(weights, axis=0, keepdims=True)
        weight_refs[t % 2][...] = weights.astype(jnp.bfloat16)

    def spread(t):
        k, i, p = pieces[t]
        at = slice(p * span, (p + 1) * span)
        c = k * parts + i
        acc = jnp.dot(flip_ref[k], weight_refs[t % 2][...], preferred_element_type=jnp.float32)
        total = totals[t]
        if not first:
            factor = jnp.exp2(old_top[c, :, at] - tops[t])
            total = total + old_total[c, :, at] * factor
            acc = acc + old_acc[c, :, at] * factor
        if last:
            done = (acc * (1.0 / total)).T.astype(jnp.bfloat16)
            for j in range(pair):
                outs[0][i * rows : (i + 1) * rows, head_cols(k, p, j)] = done[
                    j * rows : (j + 1) * rows, :
                ]
        else:
            outs[0][c, :, at] = tops[t]
            outs[1][c, :, at] = total
            outs[2][c, :, at] = acc

    for t in range(len(pieces) + 2):
        if t < len(pieces):
            score(t)
        if t >= 2:
            spread(t - 2)
        if 1 <= t <= len(pieces):
            weigh(t - 1)


def attend(order, queries, blocks, state, last, kv_heads):
    tokens, width = queries.shape
    parts = order.shape[0]
    rows = tokens // parts
    heads = width // kv_heads // HEAD_SIZE
    span = math.gcd(heads, 2) * rows
    scale = math.log2(math.e) / math.sqrt(HEAD_SIZE)
    first = state is None
    seen = sum(block.shape[0] - TAIL for block in blocks)
    pairs = tokens * width // HEAD_SIZE * seen
    whole = pl.BlockSpec(memory_space=pltpu.VMEM)
    combos = kv_heads * parts
    state_shape = [
        jax.ShapeDtypeStruct((combos, 1, heads * rows), jnp.float32),
        jax.ShapeDtypeStruct((combos, 1, heads * rows), jnp.float32),
        jax.ShapeDtypeStruct((combos, HEAD_SIZE, heads * rows), jnp.float32),
    ]
    return pl.pallas_call(
        functools.partial(attend_kernel, len(blocks), first, last, scale, kv_heads, span),
        in_specs=[pl.BlockSpec(memory_space=pltpu.SMEM)]
        + [whole] * (1 + len(blocks) + (0 if first else 3)),
        out_specs=[whole] if last else [whole] * 3,
        out_shape=[jax.ShapeDtypeStruct(queries.shape, jnp.bfloat16)] if last else state_shape,
        scratch_shapes=[
            pltpu.VMEM((parts, seen, rows), jnp.float32),
            pltpu.VMEM((kv_heads, HEAD_SIZE, seen), jnp.bfloat16),
        ]
        + [pltpu.VMEM((seen, span), jnp.float32)] * 2
        + [pltpu.VMEM((seen, span), jnp.bfloat16)] * 2,
        compiler_params=pltpu.CompilerParams(vmem_limit_bytes=VMEM_LIMIT),
        cost_estimate=pl.CostEstimate(
            flops=4 * pairs * HEAD_SIZE, bytes_accessed=4 * pairs, transcendentals=pairs
        ),
    )(order, queries, *blocks, *(() if first else state))


def project_kernel(at_ref, a_ref, w_ref, *refs):
    send_ref, keep_ref = refs[-2:]
    wide = math.gcd(send_ref.shape[1], 256)
    for out, which in ((send_ref, 0), (keep_ref, 1)):
        for tile in range(out.shape[1] // wide):
            column = pl.multiple_of(at_ref[which] + tile * wide, wide)
            out[:, tile * wide : (tile + 1) * wide] = jnp.dot(
                a_ref[...], w_ref[:, pl.ds(column, wide)], preferred_element_type=jnp.float32
            ).astype(out.dtype)


def project(attended, weight, send_at, keep_at, columns, after):
    tokens, depth = attended.shape
    whole = pl.BlockSpec(memory_space=pltpu.VMEM)
    return pl.pallas_call(
        project_kernel,
        in_specs=[pl.BlockSpec(memory_space=pltpu.SMEM), whole, whole]
        + [pl.BlockSpec(memory_space=pl.ANY)] * len(after),
        out_specs=[whole] * 2,
        out_shape=[
            jax.ShapeDtypeStruct((tokens, columns), jnp.bfloat16),
            jax.ShapeDtypeStruct((tokens, columns), jnp.float32),
        ],
        compiler_params=pltpu.CompilerParams(vmem_limit_bytes=VMEM_LIMIT),
        cost_estimate=pl.CostEstimate(
            flops=4 * tokens * depth * columns,
            bytes_accessed=4 * depth * columns,
            transcendentals=0,
        ),
    )(jnp.stack([send_at, keep_at]).astype(jnp.int32), attended, weight, *after)


def shards(n_ctx, n_tp, queries, keys, values, out_weight, block_order):
    heads_dev = queries.shape[1] // HEAD_SIZE
    group_size = QUERY_HEADS // KEY_VALUE_HEADS
    kv_heads = max(1, heads_dev // group_size)
    tp = lax.axis_index("tp")
    start = tp * heads_dev // group_size * HEAD_SIZE
    own_keys = lax.dynamic_slice_in_dim(keys, start, kv_heads * HEAD_SIZE, 1)
    own_values = lax.dynamic_slice_in_dim(values, start, kv_heads * HEAD_SIZE, 1)
    pieces = []
    for head in range(kv_heads):
        at = slice(head * HEAD_SIZE, (head + 1) * HEAD_SIZE)
        pieces += [own_keys[:, at], own_values[:, at]]
    body = jnp.concatenate(pieces, axis=1)
    digits = jnp.stack([block_order // DIGIT, block_order % DIGIT], axis=1).reshape(-1)
    digits = jnp.pad(digits, (0, TAIL - digits.shape[0])).astype(jnp.bfloat16)
    tail = jnp.broadcast_to(digits[:, None], (TAIL, body.shape[1]))
    own = jnp.concatenate([body, tail], axis=0)

    inner = math.gcd(n_ctx, 2)
    outer = n_ctx // inner

    def along_outer(block, k):
        pairs = [
            (o * inner + i, (o + k) % outer * inner + i) for o in range(outer) for i in range(inner)
        ]
        return lax.ppermute(block, "ctx", pairs)

    def along_inner(block):
        found = []
        for k in range(1, inner):
            pairs = [
                (o * inner + i, o * inner + (i + k) % inner)
                for o in range(outer)
                for i in range(inner)
            ]
            found.append(lax.ppermute(block, "ctx", pairs))
        return found

    steps = []
    for k in range(1, outer // 2 + 1):
        steps.append([k] if 2 * k == outer else [k, outer - k])
    columns = [[along_outer(own, k) for k in step] for step in steps]
    arrived = along_inner(own)
    before = []
    for step, blocks in zip(steps, columns):
        arrived += before + blocks
        before = []
        for k, block in zip(step, blocks):
            before += along_inner(block)
    arrived += before

    stages = [[own]]
    stages += [arrived[i : min(i + 3, len(arrived) - 1)] for i in range(0, len(arrived) - 1, 3)]
    stages += [arrived[-1:]] if arrived else []
    state = None
    for index, blocks in enumerate(stages):
        state = attend(
            block_order, queries, blocks, state, index == len(stages) - 1, kv_heads
        )
    attended = state[0]

    share = out_weight.shape[1] // n_tp
    cores = math.gcd(n_tp, 2)
    groups = n_tp // cores
    core, group = tp % cores, tp // cores

    def to_core(x):
        pairs = [(t, t // cores * cores + (t + 1) % cores) for t in range(n_tp)]
        return lax.ppermute(x, "tp", pairs)

    def to_group(x, r):
        pairs = [(t, (t + r * cores) % n_tp) for t in range(n_tp)]
        return lax.ppermute(x, "tp", pairs)

    def projected(r, at, width, after):
        to = (group + r) % groups * cores
        return project(
            attended,
            out_weight,
            (to + (core + 1) % cores) * share + at,
            (to + core) * share + at,
            width,
            after,
        )

    cuts = 2 if groups == 2 else 1
    width = share // cuts
    after = ()
    partial = []
    for cut in range(cuts):
        for r in range(1, groups):
            send, keep = projected(r, cut * width, width, after)
            after = (send,)
            partial.append((cut, r, to_core(send) if cores > 1 else None, keep))
    arriving = [[] for _ in range(cuts)]
    for cut, r, other, keep in partial:
        if other is not None:
            keep = keep + other.astype(jnp.float32)
        summed = keep.astype(jnp.bfloat16)
        after += (summed,)
        arriving[cut].append(to_group(summed, r))
    send, mine = projected(0, 0, share, after)
    if cores > 1:
        mine = mine + to_core(send).astype(jnp.float32)
    result = []
    for cut in range(cuts):
        total = mine[:, cut * width : (cut + 1) * width]
        for x in arriving[cut]:
            total = total + x.astype(jnp.float32)
        result.append(total.astype(jnp.bfloat16))
    return jnp.concatenate(result, axis=1)


def solution(mesh):
    in_specs = (P("ctx", "tp"), P("ctx", None), P("ctx", None), P("tp", None), P("ctx"))
    out_specs = P("ctx", "tp")

    def layer(*args):
        return shards(mesh.shape["ctx"], mesh.shape["tp"], *args)

    return jax.shard_map(
        layer, mesh=mesh, in_specs=in_specs, out_specs=out_specs, check_vma=False
    )
```

```python
import functools
import math

import jax
import jax.numpy as jnp
from jax import lax
from jax.experimental import pallas as pl
from jax.experimental.pallas import tpu as pltpu
from jax.sharding import PartitionSpec as P

QUERY_HEADS = 64
KEY_VALUE_HEADS = 8
HEAD_SIZE = 128
HIDDEN = -1e30
TAIL = 16
DIGIT = 128
NT = (((1,), (1,)), ((), ()))
VMEM_LIMIT = 16 << 20
WIDE_LIMIT = 48 << 20


def fetch_columns(at_ref, weight_ref, buffer, sem, counts):
    wide = buffer.shape[2]
    copies = []
    for run, count in enumerate(counts):
        for tile in range(count):
            column = pl.multiple_of(at_ref[run] + tile * wide, wide)
            n = len(copies)
            copies.append(
                pltpu.make_async_copy(
                    weight_ref.at[:, pl.ds(column, wide)], buffer.at[n], sem.at[n]
                )
            )
            copies[-1].start()
    return copies


def multiply_columns(rows_ref, buffer, copies, outs):
    wide = buffer.shape[2]
    n = 0
    for out in outs:
        for tile in range(out.shape[1] // wide):
            copies[n].wait()
            out[:, tile * wide : (tile + 1) * wide] = jnp.dot(
                rows_ref[...], buffer[n], preferred_element_type=jnp.float32
            ).astype(out.dtype)
            n += 1


def attend_kernel(n_blocks, first, last, scale, kv_heads, span, *refs):
    order_ref, q_ref = refs[:2]
    blocks = refs[2 : 2 + n_blocks]
    refs = refs[2 + n_blocks :]
    if not first:
        old_top, old_total, old_acc = refs[:3]
        refs = refs[3:]
    if last:
        at_ref, weight_ref = refs[:2]
        buffer, sem = refs[-2:]
        refs = refs[2:-2]
        counts = [out.shape[1] // buffer.shape[2] for out in refs[1:3]]
        copies = fetch_columns(at_ref, weight_ref, buffer, sem, counts)
    outs = refs[:3]
    bias_ref, flip_ref = refs[-6:-4]
    score_refs, weight_refs = refs[-4:-2], refs[-2:]
    parts = order_ref.shape[0]
    rows = q_ref.shape[0] // parts
    heads = q_ref.shape[1] // kv_heads // HEAD_SIZE
    pair = span // rows
    lengths = [block.shape[0] - TAIL for block in blocks]
    offsets = [sum(lengths[:b]) for b in range(n_blocks)]

    key_at = lax.broadcasted_iota(jnp.int32, (rows, rows), 0).astype(jnp.float32)
    query_iota = lax.broadcasted_iota(jnp.int32, (rows, rows), 1)
    for block, length, offset in zip(blocks, lengths, offsets):
        tail = block[length : length + TAIL, 0:HEAD_SIZE].astype(jnp.float32)
        for part in range(length // rows):
            high, low = tail[2 * part : 2 * part + 1, :], tail[2 * part + 1 : 2 * part + 2, :]
            key_pos = (high * DIGIT + low)[:, 0:rows] * float(rows) + key_at
            at = slice(offset + part * rows, offset + (part + 1) * rows)
            for i in range(parts):
                query_pos = (query_iota + order_ref[i] * rows).astype(jnp.float32)
                bias_ref[i, at, :] = jnp.where(key_pos > query_pos, HIDDEN, 0.0)
        for k in range(kv_heads):
            at = slice((2 * k + 1) * HEAD_SIZE, (2 * k + 2) * HEAD_SIZE)
            flip_ref[k, :, offset : offset + length] = block[0:length, at].T

    pieces = [
        (k, i, p) for k in range(kv_heads) for i in range(parts) for p in range(heads // pair)
    ]
    tops, totals = {}, {}

    def head_cols(k, p, j):
        head = k * heads + p * pair + j
        return slice(head * HEAD_SIZE, (head + 1) * HEAD_SIZE)

    def score(t):
        k, i, p = pieces[t]
        q = jnp.concatenate(
            [q_ref[i * rows : (i + 1) * rows, head_cols(k, p, j)] for j in range(pair)], axis=0
        )
        top = None
        for block, length, offset in zip(blocks, lengths, offsets):
            key = block[0:length, 2 * k * HEAD_SIZE : (2 * k + 1) * HEAD_SIZE]
            tile = bias_ref[i, offset : offset + length, :]
            scores = lax.dot_general(key, q, NT, preferred_element_type=jnp.float32)
            scores = scores * scale + jnp.concatenate([tile] * pair, axis=1)
            score_refs[t % 2][offset : offset + length, :] = scores
            part = jnp.max(scores, axis=0, keepdims=True)
            top = part if top is None else jnp.maximum(top, part)
        if not first:
            top = jnp.maximum(top, old_top[k * parts + i, :, p * span : (p + 1) * span])
        tops[t] = top

    def weigh(t):
        weights = jnp.exp2(score_refs[t % 2][...] - tops[t])
        totals[t] = jnp.sum(weights, axis=0, keepdims=True)
        weight_refs[t % 2][...] = weights.astype(jnp.bfloat16)

    def spread(t):
        k, i, p = pieces[t]
        at = slice(p * span, (p + 1) * span)
        c = k * parts + i
        acc = jnp.dot(flip_ref[k], weight_refs[t % 2][...], preferred_element_type=jnp.float32)
        total = totals[t]
        if not first:
            factor = jnp.exp2(old_top[c, :, at] - tops[t])
            total = total + old_total[c, :, at] * factor
            acc = acc + old_acc[c, :, at] * factor
        if last:
            done = (acc * (1.0 / total)).T.astype(jnp.bfloat16)
            for j in range(pair):
                outs[0][i * rows : (i + 1) * rows, head_cols(k, p, j)] = done[
                    j * rows : (j + 1) * rows, :
                ]
        else:
            outs[0][c, :, at] = tops[t]
            outs[1][c, :, at] = total
            outs[2][c, :, at] = acc

    for t in range(len(pieces) + 2):
        if t < len(pieces):
            score(t)
        if t >= 2:
            spread(t - 2)
        if 1 <= t <= len(pieces):
            weigh(t - 1)
    if last:
        multiply_columns(outs[0], buffer, copies, outs[1:3])


def product_shapes(tokens, columns):
    return [
        jax.ShapeDtypeStruct((tokens, columns), jnp.bfloat16),
        jax.ShapeDtypeStruct((tokens, columns), jnp.float32),
    ]


def column_scratch(depth, columns):
    wide = math.gcd(columns, 256)
    tiles = 2 * columns // wide
    return [pltpu.VMEM((tiles, depth, wide), jnp.bfloat16), pltpu.SemaphoreType.DMA((tiles,))]


def attend(order, queries, blocks, state, kv_heads, then=None):
    tokens, width = queries.shape
    parts = order.shape[0]
    rows = tokens // parts
    heads = width // kv_heads // HEAD_SIZE
    span = math.gcd(heads, 2) * rows
    scale = math.log2(math.e) / math.sqrt(HEAD_SIZE)
    first, last = state is None, then is not None
    seen = sum(block.shape[0] - TAIL for block in blocks)
    pairs = tokens * width // HEAD_SIZE * seen
    whole = pl.BlockSpec(memory_space=pltpu.VMEM)
    scalars = pl.BlockSpec(memory_space=pltpu.SMEM)
    combos = kv_heads * parts
    operands = [order, queries, *blocks, *(() if first else state)]
    in_specs = [scalars] + [whole] * (len(operands) - 1)
    scratch = [
        pltpu.VMEM((parts, seen, rows), jnp.float32),
        pltpu.VMEM((kv_heads, HEAD_SIZE, seen), jnp.bfloat16),
    ]
    scratch += [pltpu.VMEM((seen, span), jnp.float32)] * 2
    scratch += [pltpu.VMEM((seen, span), jnp.bfloat16)] * 2
    flops = 4 * pairs * HEAD_SIZE
    if last:
        at, weight, columns = then
        operands += [at, weight]
        in_specs += [scalars, pl.BlockSpec(memory_space=pl.ANY)]
        out_shape = [jax.ShapeDtypeStruct(queries.shape, jnp.bfloat16)]
        out_shape += product_shapes(tokens, columns)
        scratch += column_scratch(width, columns)
        flops += 4 * tokens * width * columns
    else:
        out_shape = [
            jax.ShapeDtypeStruct((combos, 1, heads * rows), jnp.float32),
            jax.ShapeDtypeStruct((combos, 1, heads * rows), jnp.float32),
            jax.ShapeDtypeStruct((combos, HEAD_SIZE, heads * rows), jnp.float32),
        ]
    return pl.pallas_call(
        functools.partial(attend_kernel, len(blocks), first, last, scale, kv_heads, span),
        in_specs=in_specs,
        out_specs=[whole] * len(out_shape),
        out_shape=out_shape,
        scratch_shapes=scratch,
        compiler_params=pltpu.CompilerParams(vmem_limit_bytes=WIDE_LIMIT if last else VMEM_LIMIT),
        cost_estimate=pl.CostEstimate(
            flops=flops, bytes_accessed=4 * pairs, transcendentals=pairs
        ),
    )(*operands)


def project_kernel(at_ref, rows_ref, weight_ref, *refs):
    send_ref, keep_ref, buffer, sem = refs[-4:]
    counts = [out.shape[1] // buffer.shape[2] for out in (send_ref, keep_ref)]
    copies = fetch_columns(at_ref, weight_ref, buffer, sem, counts)
    multiply_columns(rows_ref, buffer, copies, (send_ref, keep_ref))


def project(at, attended, weight, columns, after):
    tokens, depth = attended.shape
    whole = pl.BlockSpec(memory_space=pltpu.VMEM)
    unread = pl.BlockSpec(memory_space=pl.ANY)
    return pl.pallas_call(
        project_kernel,
        in_specs=[pl.BlockSpec(memory_space=pltpu.SMEM), whole, unread] + [unread] * len(after),
        out_specs=[whole] * 2,
        out_shape=product_shapes(tokens, columns),
        scratch_shapes=column_scratch(depth, columns),
        compiler_params=pltpu.CompilerParams(vmem_limit_bytes=WIDE_LIMIT),
        cost_estimate=pl.CostEstimate(
            flops=4 * tokens * depth * columns,
            bytes_accessed=4 * depth * columns,
            transcendentals=0,
        ),
    )(at, attended, weight, *after)


def shards(n_ctx, n_tp, queries, keys, values, out_weight, block_order):
    heads_dev = queries.shape[1] // HEAD_SIZE
    group_size = QUERY_HEADS // KEY_VALUE_HEADS
    kv_heads = max(1, heads_dev // group_size)
    tp = lax.axis_index("tp")
    start = tp * heads_dev // group_size * HEAD_SIZE
    own_keys = lax.dynamic_slice_in_dim(keys, start, kv_heads * HEAD_SIZE, 1)
    own_values = lax.dynamic_slice_in_dim(values, start, kv_heads * HEAD_SIZE, 1)
    pieces = []
    for head in range(kv_heads):
        at = slice(head * HEAD_SIZE, (head + 1) * HEAD_SIZE)
        pieces += [own_keys[:, at], own_values[:, at]]
    body = jnp.concatenate(pieces, axis=1)
    digits = jnp.stack([block_order // DIGIT, block_order % DIGIT], axis=1).reshape(-1)
    digits = jnp.pad(digits, (0, TAIL - digits.shape[0])).astype(jnp.bfloat16)
    tail = jnp.broadcast_to(digits[:, None], (TAIL, body.shape[1]))
    own = jnp.concatenate([body, tail], axis=0)

    inner = math.gcd(n_ctx, 2)
    outer = n_ctx // inner

    def along_outer(block, k):
        pairs = [
            (o * inner + i, (o + k) % outer * inner + i) for o in range(outer) for i in range(inner)
        ]
        return lax.ppermute(block, "ctx", pairs)

    def along_inner(block):
        found = []
        for k in range(1, inner):
            pairs = [
                (o * inner + i, o * inner + (i + k) % inner)
                for o in range(outer)
                for i in range(inner)
            ]
            found.append(lax.ppermute(block, "ctx", pairs))
        return found

    steps = []
    for k in range(1, outer // 2 + 1):
        steps.append([k] if 2 * k == outer else [k, outer - k])
    columns = [[along_outer(own, k) for k in step] for step in steps]
    arrived = along_inner(own)
    before = []
    for step, blocks in zip(steps, columns):
        arrived += before + blocks
        before = []
        for k, block in zip(step, blocks):
            before += along_inner(block)
    arrived += before

    stages = [[own]]
    stages += [arrived[i : min(i + 3, len(arrived) - 1)] for i in range(0, len(arrived) - 1, 3)]
    stages += [arrived[-1:]] if arrived else []
    share = out_weight.shape[1] // n_tp
    cores = math.gcd(n_tp, 2)
    groups = n_tp // cores
    core, group = tp % cores, tp // cores
    cuts = 2 if groups == 2 else 1
    width = share // cuts
    jobs = [(cut, r) for cut in range(cuts) for r in range(1, groups)]

    def begins(cut, r):
        to = (group + r) % groups * cores
        at = jnp.stack([to + (core + 1) % cores, to + core]) * share + cut * width
        return at.astype(jnp.int32)

    def to_core(x):
        pairs = [(t, t // cores * cores + (t + 1) % cores) for t in range(n_tp)]
        return lax.ppermute(x, "tp", pairs)

    def to_group(x, r):
        pairs = [(t, (t + r * cores) % n_tp) for t in range(n_tp)]
        return lax.ppermute(x, "tp", pairs)

    state = None
    for blocks in stages[:-1]:
        state = attend(block_order, queries, blocks, state, kv_heads)
    first = jobs[0] if jobs else (0, 0)
    attended, send, keep = attend(
        block_order,
        queries,
        stages[-1],
        state,
        kv_heads,
        (begins(*first), out_weight, width),
    )

    partial = []
    for name, (cut, r) in enumerate(jobs):
        if name > 0:
            send, keep = project(begins(cut, r), attended, out_weight, width, (send,))
        partial.append((to_core(send) if cores > 1 else None, keep))
    arriving = [[] for _ in range(cuts)]
    after = (send,)
    for (cut, r), (other, keep) in zip(jobs, partial):
        if other is not None:
            keep = keep + other.astype(jnp.float32)
        summed = keep.astype(jnp.bfloat16)
        after += (summed,)
        arriving[cut].append(to_group(summed, r))
    send, mine = project(begins(0, 0), attended, out_weight, share, after)
    if cores > 1:
        mine = mine + to_core(send).astype(jnp.float32)
    result = []
    for cut in range(cuts):
        total = mine[:, cut * width : (cut + 1) * width]
        for x in arriving[cut]:
            total = total + x.astype(jnp.float32)
        result.append(total.astype(jnp.bfloat16))
    return jnp.concatenate(result, axis=1)


def solution(mesh):
    in_specs = (P("ctx", "tp"), P("ctx", None), P("ctx", None), P("tp", None), P("ctx"))
    out_specs = P("ctx", "tp")

    def layer(*args):
        return shards(mesh.shape["ctx"], mesh.shape["tp"], *args)

    return jax.shard_map(
        layer, mesh=mesh, in_specs=in_specs, out_specs=out_specs, check_vma=False
    )
```

```python
import functools
import math

import jax
import jax.numpy as jnp
from jax import lax
from jax.experimental import pallas as pl
from jax.experimental.pallas import tpu as pltpu
from jax.sharding import PartitionSpec as P

QUERY_HEADS = 64
KEY_VALUE_HEADS = 8
HEAD_SIZE = 128
HIDDEN = -1e30
TAIL = 16
DIGIT = 128
NT = (((1,), (1,)), ((), ()))
DEPTH = 3
VMEM_LIMIT = 16 << 20
WIDE_LIMIT = 48 << 20


WHOLE = pl.BlockSpec(memory_space=pltpu.VMEM)
SCALARS = pl.BlockSpec(memory_space=pltpu.SMEM)
UNREAD = pl.BlockSpec(memory_space=pl.ANY)


def lanes(n):
    return slice(n * HEAD_SIZE, (n + 1) * HEAD_SIZE)


def pack_kernel(kv_heads, at_ref, order_ref, keys_ref, values_ref, whole_ref, *head_refs):
    tokens = keys_ref.shape[0]
    line = lax.broadcasted_iota(jnp.int32, (TAIL, HEAD_SIZE), 0)
    tail = jnp.zeros((TAIL, HEAD_SIZE), jnp.int32)
    for part in range(order_ref.shape[0]):
        number = order_ref[part]
        tail = jnp.where(line == 2 * part, number // DIGIT, tail)
        tail = jnp.where(line == 2 * part + 1, number % DIGIT, tail)
    tail = tail.astype(jnp.float32).astype(jnp.bfloat16)
    for k in range(kv_heads):
        column = pl.multiple_of(at_ref[0] + k * HEAD_SIZE, HEAD_SIZE)
        for n, ref in enumerate((keys_ref, values_ref)):
            part = ref[:, pl.ds(column, HEAD_SIZE)]
            outs = [(whole_ref, 2 * k + n)] + [(ref, n) for ref in head_refs[k : k + 1]]
            for out, place in outs:
                out[0:tokens, lanes(place)] = part
                out[tokens : tokens + TAIL, lanes(place)] = tail


def pack(at, order, keys, values, kv_heads):
    rows = keys.shape[0] + TAIL
    out_shape = [jax.ShapeDtypeStruct((rows, 2 * kv_heads * HEAD_SIZE), jnp.bfloat16)]
    if kv_heads > 1:
        out_shape += [jax.ShapeDtypeStruct((rows, 2 * HEAD_SIZE), jnp.bfloat16)] * kv_heads
    found = pl.pallas_call(
        functools.partial(pack_kernel, kv_heads),
        in_specs=[SCALARS, SCALARS, WHOLE, WHOLE],
        out_specs=[WHOLE] * len(out_shape),
        out_shape=out_shape,
        compiler_params=pltpu.CompilerParams(vmem_limit_bytes=VMEM_LIMIT),
        cost_estimate=pl.CostEstimate(
            flops=rows * 4096, bytes_accessed=4 * rows * 1024, transcendentals=0
        ),
    )(at, order, keys, values)
    return found[0], found[1:] if kv_heads > 1 else found


class Columns:
    def __init__(self, at_ref, weight_ref, buffer, sem, outs):
        wide = buffer.shape[2]
        self.buffer = buffer
        self.copies, self.places = [], []
        for run, out in enumerate(outs):
            for tile in range(out.shape[1] // wide):
                column = pl.multiple_of(at_ref[run] + tile * wide, wide)
                n = len(self.copies)
                source = weight_ref.at[:, pl.ds(column, wide)]
                self.copies.append(pltpu.make_async_copy(source, buffer.at[n], sem.at[n]))
                self.places.append((out, slice(tile * wide, (tile + 1) * wide)))
        for copy in self.copies[:DEPTH]:
            copy.start()

    def multiply(self, rows_refs):
        for n, (copy, (out, at)) in enumerate(zip(self.copies, self.places)):
            copy.wait()
            if n + DEPTH < len(self.copies):
                self.copies[n + DEPTH].start()
            product, depth = None, 0
            for ref in rows_refs:
                held = self.buffer[n, depth : depth + ref.shape[1], :]
                part = jnp.dot(ref[...], held, preferred_element_type=jnp.float32)
                product = part if product is None else product + part
                depth += ref.shape[1]
            out[:, at] = product.astype(out.dtype)


def product_shapes(tokens, columns):
    return [
        jax.ShapeDtypeStruct((tokens, columns), jnp.bfloat16),
        jax.ShapeDtypeStruct((tokens, columns), jnp.float32),
    ]


def column_scratch(depth, columns):
    wide = math.gcd(columns, 256)
    tiles = 2 * columns // wide
    return [pltpu.VMEM((tiles, depth, wide), jnp.bfloat16), pltpu.SemaphoreType.DMA((tiles,))]


def attend_kernel(head, heads, places, first, last, earlier, scale, span, *refs):
    order_ref, q_ref = refs[:2]
    blocks = refs[2 : 2 + len(places)]
    refs = refs[2 + len(places) :]
    if not first:
        old_top, old_total, old_acc = refs[:3]
        refs = refs[3:]
    columns = None
    if earlier is not None:
        at_ref, weight_ref = refs[:2]
        earlier_refs = refs[2 : 2 + earlier]
        buffer, sem = refs[-2:]
        refs = refs[2 + earlier : -2]
        columns = Columns(at_ref, weight_ref, buffer, sem, refs[1:3])
    outs = refs[:-6]
    bias_ref, flip_ref = refs[-6:-4]
    score_refs, weight_refs = refs[-4:-2], refs[-2:]
    parts = order_ref.shape[0]
    rows = q_ref.shape[0] // parts
    pair = span // rows
    lengths = [block.shape[0] - TAIL for block in blocks]
    offsets = [sum(lengths[:b]) for b in range(len(blocks))]

    key_at = lax.broadcasted_iota(jnp.int32, (rows, rows), 0).astype(jnp.float32)
    query_iota = lax.broadcasted_iota(jnp.int32, (rows, rows), 1)
    for block, place, length, offset in zip(blocks, places, lengths, offsets):
        tail = block[length : length + TAIL, lanes(0)].astype(jnp.float32)
        for part in range(length // rows):
            high, low = tail[2 * part : 2 * part + 1, :], tail[2 * part + 1 : 2 * part + 2, :]
            key_pos = (high * DIGIT + low)[:, 0:rows] * float(rows) + key_at
            at = slice(offset + part * rows, offset + (part + 1) * rows)
            for i in range(parts):
                query_pos = (query_iota + order_ref[i] * rows).astype(jnp.float32)
                bias_ref[i, at, :] = jnp.where(key_pos > query_pos, HIDDEN, 0.0)
        flip_ref[:, offset : offset + length] = block[0:length, lanes(2 * place + 1)].T

    pieces = [(i, p) for i in range(parts) for p in range(heads // pair)]
    tops, totals = {}, {}

    def score(t):
        i, p = pieces[t]
        found = [
            q_ref[i * rows : (i + 1) * rows, lanes(head * heads + p * pair + j)]
            for j in range(pair)
        ]
        q = jnp.concatenate(found, axis=0)
        top = None
        for block, place, length, offset in zip(blocks, places, lengths, offsets):
            key = block[0:length, lanes(2 * place)]
            tile = bias_ref[i, offset : offset + length, :]
            scores = lax.dot_general(key, q, NT, preferred_element_type=jnp.float32)
            scores = scores * scale + jnp.concatenate([tile] * pair, axis=1)
            score_refs[t % 2][offset : offset + length, :] = scores
            part = jnp.max(scores, axis=0, keepdims=True)
            top = part if top is None else jnp.maximum(top, part)
        if not first:
            top = jnp.maximum(top, old_top[i, :, p * span : (p + 1) * span])
        tops[t] = top

    def weigh(t):
        weights = jnp.exp2(score_refs[t % 2][...] - tops[t])
        totals[t] = jnp.sum(weights, axis=0, keepdims=True)
        weight_refs[t % 2][...] = weights.astype(jnp.bfloat16)

    def spread(t):
        i, p = pieces[t]
        at = slice(p * span, (p + 1) * span)
        acc = jnp.dot(flip_ref[...], weight_refs[t % 2][...], preferred_element_type=jnp.float32)
        total = totals[t]
        if not first:
            factor = jnp.exp2(old_top[i, :, at] - tops[t])
            total = total + old_total[i, :, at] * factor
            acc = acc + old_acc[i, :, at] * factor
        if last:
            done = (acc * (1.0 / total)).T.astype(jnp.bfloat16)
            for j in range(pair):
                outs[0][i * rows : (i + 1) * rows, lanes(p * pair + j)] = done[
                    j * rows : (j + 1) * rows, :
                ]
        else:
            outs[0][i, :, at] = tops[t]
            outs[1][i, :, at] = total
            outs[2][i, :, at] = acc

    for t in range(len(pieces) + 2):
        if t < len(pieces):
            score(t)
        if t >= 2:
            spread(t - 2)
        if 1 <= t <= len(pieces):
            weigh(t - 1)
    if columns is not None:
        columns.multiply((*earlier_refs, outs[0]))


def attend(order, queries, kv_heads, head, blocks, state, last=False, then=None):
    tokens, width = queries.shape
    parts = order.shape[0]
    rows = tokens // parts
    heads = width // kv_heads // HEAD_SIZE
    span = math.gcd(heads, 2) * rows
    scale = math.log2(math.e) / math.sqrt(HEAD_SIZE)
    first = state is None
    arrays = [array for array, _ in blocks]
    places = [place for _, place in blocks]
    seen = sum(array.shape[0] - TAIL for array in arrays)
    pairs = tokens * heads * seen
    operands = [order, queries, *arrays, *(() if first else state)]
    in_specs = [SCALARS] + [WHOLE] * (len(operands) - 1)
    scratch = [
        pltpu.VMEM((parts, seen, rows), jnp.float32),
        pltpu.VMEM((HEAD_SIZE, seen), jnp.bfloat16),
    ]
    scratch += [pltpu.VMEM((seen, span), jnp.float32)] * 2
    scratch += [pltpu.VMEM((seen, span), jnp.bfloat16)] * 2
    flops = 4 * pairs * HEAD_SIZE
    if last:
        out_shape = [jax.ShapeDtypeStruct((tokens, heads * HEAD_SIZE), jnp.bfloat16)]
    else:
        out_shape = [
            jax.ShapeDtypeStruct((parts, 1, heads * rows), jnp.float32),
            jax.ShapeDtypeStruct((parts, 1, heads * rows), jnp.float32),
            jax.ShapeDtypeStruct((parts, HEAD_SIZE, heads * rows), jnp.float32),
        ]
    earlier = None
    if then is not None:
        at, weight, columns, done = then
        earlier = len(done)
        operands += [at, weight, *done]
        in_specs += [SCALARS, UNREAD] + [WHOLE] * earlier
        out_shape += product_shapes(tokens, columns)
        scratch += column_scratch(width, columns)
        flops += 4 * tokens * width * columns
    return pl.pallas_call(
        functools.partial(
            attend_kernel, head, heads, places, first, last, earlier, scale, span
        ),
        in_specs=in_specs,
        out_specs=[WHOLE] * len(out_shape),
        out_shape=out_shape,
        scratch_shapes=scratch,
        compiler_params=pltpu.CompilerParams(
            vmem_limit_bytes=VMEM_LIMIT if then is None else WIDE_LIMIT,
        ),
        cost_estimate=pl.CostEstimate(
            flops=flops, bytes_accessed=4 * pairs, transcendentals=pairs
        ),
    )(*operands)


def project_kernel(n_rows, at_ref, weight_ref, *refs):
    send_ref, keep_ref, buffer, sem = refs[-4:]
    columns = Columns(at_ref, weight_ref, buffer, sem, (send_ref, keep_ref))
    columns.multiply(refs[:n_rows])


def project(at, attended, weight, columns, after):
    tokens, depth = attended[0].shape[0], weight.shape[0]
    return pl.pallas_call(
        functools.partial(project_kernel, len(attended)),
        in_specs=[SCALARS, UNREAD] + [WHOLE] * len(attended) + [UNREAD] * len(after),
        out_specs=[WHOLE] * 2,
        out_shape=product_shapes(tokens, columns),
        scratch_shapes=column_scratch(depth, columns),
        compiler_params=pltpu.CompilerParams(vmem_limit_bytes=WIDE_LIMIT),
        cost_estimate=pl.CostEstimate(
            flops=4 * tokens * depth * columns,
            bytes_accessed=4 * depth * columns,
            transcendentals=0,
        ),
    )(at, weight, *attended, *after)


def shards(n_ctx, n_tp, queries, keys, values, out_weight, block_order):
    heads_dev = queries.shape[1] // HEAD_SIZE
    group_size = QUERY_HEADS // KEY_VALUE_HEADS
    kv_heads = max(1, heads_dev // group_size)
    tp = lax.axis_index("tp")
    start = (tp * heads_dev // group_size * HEAD_SIZE).astype(jnp.int32)
    own, own_heads = pack(start[None], block_order, keys, values, kv_heads)

    inner = math.gcd(n_ctx, 2)
    outer = n_ctx // inner

    def along_outer(block, k):
        pairs = [
            (o * inner + i, (o + k) % outer * inner + i) for o in range(outer) for i in range(inner)
        ]
        return lax.ppermute(block, "ctx", pairs)

    def along_inner(block):
        found = []
        for k in range(1, inner):
            pairs = [
                (o * inner + i, o * inner + (i + k) % inner)
                for o in range(outer)
                for i in range(inner)
            ]
            found.append(lax.ppermute(block, "ctx", pairs))
        return found

    half = outer // 2
    moved = {}
    for k in range(1, half):
        for shift in (k, outer - k):
            moved[shift] = along_outer(own, shift)
    split = [along_outer(x, half) for x in own_heads] if half else []
    arrived = along_inner(own)
    before = []
    for k in range(1, half):
        for shift in (k, outer - k):
            arrived.append(moved[shift])
        arrived += before
        before = []
        for shift in (k, outer - k):
            before += along_inner(moved[shift])
    arrived += before
    final = [along_inner(x) for x in split]

    share = out_weight.shape[1] // n_tp
    cores = math.gcd(n_tp, 2)
    groups = n_tp // cores
    core, group = tp % cores, tp // cores
    cuts = [0, share // 4, share] if groups == 2 else [0, share]
    jobs = [(cut, r) for cut in range(len(cuts) - 1) for r in range(1, groups)]

    def begins(cut, r):
        to = (group + r) % groups * cores
        at = jnp.stack([to + (core + 1) % cores, to + core]) * share + cuts[cut]
        return at.astype(jnp.int32)

    def to_core(x):
        pairs = [(t, t // cores * cores + (t + 1) % cores) for t in range(n_tp)]
        return lax.ppermute(x, "tp", pairs)

    def to_group(x, r):
        pairs = [(t, (t + r * cores) % n_tp) for t in range(n_tp)]
        return lax.ppermute(x, "tp", pairs)

    tail, tail_at = (jobs[0], cuts[jobs[0][0] + 1] - cuts[jobs[0][0]]) if jobs else ((0, 0), share)
    attended = []
    batch = 3
    for head in range(kv_heads):
        stages = [[(own, head)]]
        stages += [
            [(x, head) for x in arrived[i : i + batch]] for i in range(0, len(arrived), batch)
        ]
        if split:
            if len(stages[-1]) < batch:
                stages[-1] = stages[-1] + [(split[head], 0)]
            else:
                stages.append([(split[head], 0)])
            stages += [[(x, 0)] for x in final[head]]
        state = None
        for index, blocks in enumerate(stages):
            last = index == len(stages) - 1
            then = None
            if last and head == kv_heads - 1:
                then = (begins(*tail), out_weight, tail_at, attended)
            state = attend(block_order, queries, kv_heads, head, blocks, state, last, then)
        attended = attended + [state[0]]
    send, keep = state[1:]

    partial = []
    for name, (cut, r) in enumerate(jobs):
        if name > 0:
            send, keep = project(
                begins(cut, r), attended, out_weight, cuts[cut + 1] - cuts[cut], (send,)
            )
        partial.append((to_core(send) if cores > 1 else None, keep))
    arriving = [[] for _ in cuts[1:]]
    after = (send,)
    for (cut, r), (other, keep) in zip(jobs, partial):
        if other is not None:
            keep = keep + other.astype(jnp.float32)
        summed = keep.astype(jnp.bfloat16)
        after += (summed,)
        arriving[cut].append(to_group(summed, r))
    if jobs:
        send, keep = project(begins(0, 0), attended, out_weight, share, after)
    mine = keep
    if cores > 1:
        mine = mine + to_core(send).astype(jnp.float32)
    result = []
    for cut, others in enumerate(arriving):
        total = mine[:, cuts[cut] : cuts[cut + 1]]
        for x in others:
            total = total + x.astype(jnp.float32)
        result.append(total.astype(jnp.bfloat16))
    return jnp.concatenate(result, axis=1)


def solution(mesh):
    in_specs = (P("ctx", "tp"), P("ctx", None), P("ctx", None), P("tp", None), P("ctx"))
    out_specs = P("ctx", "tp")

    def layer(*args):
        return shards(mesh.shape["ctx"], mesh.shape["tp"], *args)

    return jax.shard_map(
        layer, mesh=mesh, in_specs=in_specs, out_specs=out_specs, check_vma=False
    )
```

```python
import functools
import math

import jax
import jax.numpy as jnp
from jax import lax
from jax.experimental import pallas as pl
from jax.experimental.pallas import tpu as pltpu
from jax.sharding import PartitionSpec as P

QUERY_HEADS = 64
KEY_VALUE_HEADS = 8
HEAD_SIZE = 128
HIDDEN = -1e30
TAIL = 16
DIGIT = 128
NT = (((1,), (1,)), ((), ()))
DEPTH = 3
VMEM_LIMIT = 16 << 20
WIDE_LIMIT = 48 << 20


def fetch_columns(at_ref, weight_ref, buffer, sem, counts, started=None):
    wide = buffer.shape[2]
    copies = []
    for run, count in enumerate(counts):
        for tile in range(count):
            column = pl.multiple_of(at_ref[run] + tile * wide, wide)
            n = len(copies)
            copies.append(
                pltpu.make_async_copy(
                    weight_ref.at[:, pl.ds(column, wide)], buffer.at[n], sem.at[n]
                )
            )
    for copy in copies[:started]:
        copy.start()
    return copies


def multiply_columns(rows_ref, buffer, copies, outs):
    wide = buffer.shape[2]
    n = 0
    for out in outs:
        for tile in range(out.shape[1] // wide):
            if copies is not None:
                copies[n].wait()
                if n + DEPTH < len(copies):
                    copies[n + DEPTH].start()
            out[:, tile * wide : (tile + 1) * wide] = jnp.dot(
                rows_ref[...], buffer[n], preferred_element_type=jnp.float32
            ).astype(out.dtype)
            n += 1


def attend_kernel(halves, first, last, scale, kv_heads, span, *refs):
    n_blocks = len(halves)
    order_ref, q_ref = refs[:2]
    blocks, refs = [], refs[2:]
    for count in halves:
        blocks.append(refs[:count])
        refs = refs[count:]
    if not first:
        old_top, old_total, old_acc = refs[:3]
        refs = refs[3:]
    if last:
        at_ref, weight_ref = refs[:2]
        buffer, sem = refs[-2:]
        refs = refs[2:-2]
        products = refs[1:-7]
        counts = [out.shape[1] // buffer.shape[2] for out in products]
        copies = fetch_columns(at_ref, weight_ref, buffer, sem, counts)
    outs = refs[:3]
    merged_ref, bias_ref, flip_ref = refs[-7:-4]
    score_refs, weight_refs = refs[-4:-2], refs[-2:]
    parts = order_ref.shape[0]
    rows = q_ref.shape[0] // parts
    heads = q_ref.shape[1] // kv_heads // HEAD_SIZE
    pair = span // rows
    for b, found in enumerate(blocks):
        if len(found) == 2:
            merged_ref[...] = found[0][...] + found[1][...]
            blocks[b] = merged_ref
        else:
            blocks[b] = found[0]
    lengths = [block.shape[0] - TAIL for block in blocks]
    offsets = [sum(lengths[:b]) for b in range(n_blocks)]

    key_at = lax.broadcasted_iota(jnp.int32, (rows, rows), 0).astype(jnp.float32)
    query_iota = lax.broadcasted_iota(jnp.int32, (rows, rows), 1)
    for block, length, offset in zip(blocks, lengths, offsets):
        tail = block[length : length + TAIL, 0:HEAD_SIZE].astype(jnp.float32)
        for part in range(length // rows):
            high, low = tail[2 * part : 2 * part + 1, :], tail[2 * part + 1 : 2 * part + 2, :]
            key_pos = (high * DIGIT + low)[:, 0:rows] * float(rows) + key_at
            at = slice(offset + part * rows, offset + (part + 1) * rows)
            for i in range(parts):
                query_pos = (query_iota + order_ref[i] * rows).astype(jnp.float32)
                bias_ref[i, at, :] = jnp.where(key_pos > query_pos, HIDDEN, 0.0)
        for k in range(kv_heads):
            at = slice((2 * k + 1) * HEAD_SIZE, (2 * k + 2) * HEAD_SIZE)
            flip_ref[k, :, offset : offset + length] = block[0:length, at].T

    pieces = [
        (k, i, p) for k in range(kv_heads) for i in range(parts) for p in range(heads // pair)
    ]
    tops, totals = {}, {}

    def head_cols(k, p, j):
        head = k * heads + p * pair + j
        return slice(head * HEAD_SIZE, (head + 1) * HEAD_SIZE)

    def score(t):
        k, i, p = pieces[t]
        q = jnp.concatenate(
            [q_ref[i * rows : (i + 1) * rows, head_cols(k, p, j)] for j in range(pair)], axis=0
        )
        top = None
        for block, length, offset in zip(blocks, lengths, offsets):
            key = block[0:length, 2 * k * HEAD_SIZE : (2 * k + 1) * HEAD_SIZE]
            tile = bias_ref[i, offset : offset + length, :]
            scores = lax.dot_general(key, q, NT, preferred_element_type=jnp.float32)
            scores = scores * scale + jnp.concatenate([tile] * pair, axis=1)
            score_refs[t % 2][offset : offset + length, :] = scores
            part = jnp.max(scores, axis=0, keepdims=True)
            top = part if top is None else jnp.maximum(top, part)
        if not first:
            top = jnp.maximum(top, old_top[k * parts + i, :, p * span : (p + 1) * span])
        tops[t] = top

    def weigh(t):
        weights = jnp.exp2(score_refs[t % 2][...] - tops[t])
        totals[t] = jnp.sum(weights, axis=0, keepdims=True)
        weight_refs[t % 2][...] = weights.astype(jnp.bfloat16)

    def spread(t):
        k, i, p = pieces[t]
        at = slice(p * span, (p + 1) * span)
        c = k * parts + i
        acc = jnp.dot(flip_ref[k], weight_refs[t % 2][...], preferred_element_type=jnp.float32)
        total = totals[t]
        if not first:
            factor = jnp.exp2(old_top[c, :, at] - tops[t])
            total = total + old_total[c, :, at] * factor
            acc = acc + old_acc[c, :, at] * factor
        if last:
            done = (acc * (1.0 / total)).T.astype(jnp.bfloat16)
            for j in range(pair):
                outs[0][i * rows : (i + 1) * rows, head_cols(k, p, j)] = done[
                    j * rows : (j + 1) * rows, :
                ]
        else:
            outs[0][c, :, at] = tops[t]
            outs[1][c, :, at] = total
            outs[2][c, :, at] = acc

    for t in range(len(pieces) + 2):
        if t < len(pieces):
            score(t)
        if t >= 2:
            spread(t - 2)
        if 1 <= t <= len(pieces):
            weigh(t - 1)
    if last:
        for copy in copies:
            copy.wait()
        multiply_columns(outs[0], buffer, None, products)


def product_shapes(tokens, widths):
    found = []
    for width in widths:
        found.append(jax.ShapeDtypeStruct((tokens, width), jnp.bfloat16))
        found.append(jax.ShapeDtypeStruct((tokens, width), jnp.float32))
    return found


def column_scratch(depth, widths):
    wide = math.gcd(256, *widths)
    tiles = 2 * sum(widths) // wide
    return [pltpu.VMEM((tiles, depth, wide), jnp.bfloat16), pltpu.SemaphoreType.DMA((tiles,))]


def attend(order, queries, blocks, state, kv_heads, then=None):
    tokens, width = queries.shape
    parts = order.shape[0]
    rows = tokens // parts
    heads = width // kv_heads // HEAD_SIZE
    span = math.gcd(heads, 2) * rows
    scale = math.log2(math.e) / math.sqrt(HEAD_SIZE)
    first, last = state is None, then is not None
    seen = sum(block[0].shape[0] - TAIL for block in blocks)
    pairs = tokens * width // HEAD_SIZE * seen
    whole = pl.BlockSpec(memory_space=pltpu.VMEM)
    scalars = pl.BlockSpec(memory_space=pltpu.SMEM)
    combos = kv_heads * parts
    halves = [len(block) for block in blocks]
    arrays = [array for block in blocks for array in block]
    operands = [order, queries, *arrays, *(() if first else state)]
    in_specs = [scalars] + [whole] * (len(operands) - 1)
    scratch = [
        pltpu.VMEM(arrays[0].shape, arrays[0].dtype),
        pltpu.VMEM((parts, seen, rows), jnp.float32),
        pltpu.VMEM((kv_heads, HEAD_SIZE, seen), jnp.bfloat16),
    ]
    scratch += [pltpu.VMEM((seen, span), jnp.float32)] * 2
    scratch += [pltpu.VMEM((seen, span), jnp.bfloat16)] * 2
    flops = 4 * pairs * HEAD_SIZE
    if last:
        at, weight, widths = then
        operands += [at, weight]
        in_specs += [scalars, pl.BlockSpec(memory_space=pl.ANY)]
        out_shape = [jax.ShapeDtypeStruct(queries.shape, jnp.bfloat16)]
        out_shape += product_shapes(tokens, widths)
        scratch += column_scratch(width, widths)
        flops += 4 * tokens * width * sum(widths)
    else:
        out_shape = [
            jax.ShapeDtypeStruct((combos, 1, heads * rows), jnp.float32),
            jax.ShapeDtypeStruct((combos, 1, heads * rows), jnp.float32),
            jax.ShapeDtypeStruct((combos, HEAD_SIZE, heads * rows), jnp.float32),
        ]
    return pl.pallas_call(
        functools.partial(attend_kernel, halves, first, last, scale, kv_heads, span),
        in_specs=in_specs,
        out_specs=[whole] * len(out_shape),
        out_shape=out_shape,
        scratch_shapes=scratch,
        compiler_params=pltpu.CompilerParams(vmem_limit_bytes=WIDE_LIMIT if last else VMEM_LIMIT),
        cost_estimate=pl.CostEstimate(
            flops=flops, bytes_accessed=4 * pairs, transcendentals=pairs
        ),
    )(*operands)


def project_kernel(at_ref, rows_ref, weight_ref, *refs):
    send_ref, keep_ref, buffer, sem = refs[-4:]
    counts = [out.shape[1] // buffer.shape[2] for out in (send_ref, keep_ref)]
    copies = fetch_columns(at_ref, weight_ref, buffer, sem, counts, DEPTH)
    multiply_columns(rows_ref, buffer, copies, (send_ref, keep_ref))


def project(at, attended, weight, columns, after):
    tokens, depth = attended.shape
    whole = pl.BlockSpec(memory_space=pltpu.VMEM)
    unread = pl.BlockSpec(memory_space=pl.ANY)
    return pl.pallas_call(
        project_kernel,
        in_specs=[pl.BlockSpec(memory_space=pltpu.SMEM), whole, unread] + [unread] * len(after),
        out_specs=[whole] * 2,
        out_shape=product_shapes(tokens, [columns]),
        scratch_shapes=column_scratch(depth, [columns]),
        compiler_params=pltpu.CompilerParams(vmem_limit_bytes=WIDE_LIMIT),
        cost_estimate=pl.CostEstimate(
            flops=4 * tokens * depth * columns,
            bytes_accessed=4 * depth * columns,
            transcendentals=0,
        ),
    )(at, attended, weight, *after)


def shards(n_ctx, n_tp, queries, keys, values, out_weight, block_order):
    heads_dev = queries.shape[1] // HEAD_SIZE
    group_size = QUERY_HEADS // KEY_VALUE_HEADS
    kv_heads = max(1, heads_dev // group_size)
    tp = lax.axis_index("tp")
    start = tp * heads_dev // group_size * HEAD_SIZE
    own_keys = lax.dynamic_slice_in_dim(keys, start, kv_heads * HEAD_SIZE, 1)
    own_values = lax.dynamic_slice_in_dim(values, start, kv_heads * HEAD_SIZE, 1)
    pieces = []
    for head in range(kv_heads):
        at = slice(head * HEAD_SIZE, (head + 1) * HEAD_SIZE)
        pieces += [own_keys[:, at], own_values[:, at]]
    body = jnp.concatenate(pieces, axis=1)
    digits = jnp.stack([block_order // DIGIT, block_order % DIGIT], axis=1).reshape(-1)
    digits = jnp.pad(digits, (0, TAIL - digits.shape[0])).astype(jnp.bfloat16)
    tail = jnp.broadcast_to(digits[:, None], (TAIL, body.shape[1]))
    own = jnp.concatenate([body, tail], axis=0)

    inner = math.gcd(n_ctx, 2)
    outer = n_ctx // inner

    def move(block, target):
        pairs = []
        for o in range(outer):
            for i in range(inner):
                to = target(o, i)
                if to is not None:
                    pairs.append((o * inner + i, to[0] * inner + to[1]))
        return lax.ppermute(block, "ctx", pairs)

    def cross(block, among=None):
        found = []
        for k in range(1, inner):

            def target(o, i):
                return (o, (i + k) % inner) if among is None or o in among else None

            found.append(move(block, target))
        return found

    if outer == 4:
        near = move(own, lambda o, i: (o ^ 1, i))
        mirror = move(own, lambda o, i: (3 - o, i))
        third = move(own, lambda o, i: {0: (2, i), 3: (1, i)}.get(o))
        own_crossed = cross(own)
        onward = move(mirror, lambda o, i: {2: (3, i), 1: (0, i)}.get(o))
        stages = [[(own,)], [(near,), (mirror,)] + [(x,) for x in own_crossed]]
        stages += [[(x,) for x in cross(near) + cross(mirror)]]
        stages[-1].append((third, onward))
        late = zip(cross(third, (1, 2)), cross(onward, (0, 3)))
        stages += [[pair] for pair in late]
    else:
        blocks = [own]
        for k in range(1, outer):
            blocks.append(move(own, lambda o, i: ((o + k) % outer, i)))
        arrived = blocks[1:]
        for k, block in enumerate(blocks):
            arrived += cross(block)
        arrived = [(x,) for x in arrived]
        stages = [[(own,)]]
        stages += [arrived[i : min(i + 3, len(arrived) - 1)] for i in range(0, len(arrived) - 1, 3)]
        stages += [arrived[-1:]] if arrived else []

    share = out_weight.shape[1] // n_tp
    cores = math.gcd(n_tp, 2)
    groups = n_tp // cores
    core, group = tp % cores, tp // cores
    cuts = [0, share // 4, share] if groups == 2 else [0, share]
    widths = [b - a for a, b in zip(cuts, cuts[1:])]
    jobs = [(cut, r) for r in range(1, groups) for cut in range(len(widths))]

    def begins(r, numbers):
        to = (group + r) % groups * cores
        firsts = jnp.stack([to + (core + 1) % cores, to + core]) * share
        return jnp.concatenate([firsts + cuts[n] for n in numbers]).astype(jnp.int32)

    def to_core(x):
        pairs = [(t, t // cores * cores + (t + 1) % cores) for t in range(n_tp)]
        return lax.ppermute(x, "tp", pairs)

    def to_group(x, r):
        pairs = [(t, (t + r * cores) % n_tp) for t in range(n_tp)]
        return lax.ppermute(x, "tp", pairs)

    state = None
    for blocks in stages[:-1]:
        state = attend(block_order, queries, blocks, state, kv_heads)
    together = list(range(len(widths)))
    attended, *products = attend(
        block_order,
        queries,
        stages[-1],
        state,
        kv_heads,
        (begins(min(1, groups - 1), together), out_weight, widths),
    )
    for r in range(2, groups):
        for cut in together:
            products += project(
                begins(r, [cut]), attended, out_weight, widths[cut], products[-2:-1]
            )

    arriving = [[] for _ in widths]
    after = ()
    others = [to_core(products[2 * n]) for n in range(len(jobs))] if cores > 1 else None
    for name, (cut, r) in enumerate(jobs):
        total = products[2 * name + 1]
        if cores > 1:
            total = total + others[name].astype(jnp.float32)
        total = total.astype(jnp.bfloat16)
        after += (total,)
        arriving[cut].append(to_group(total, r))
    if jobs:
        send, mine = project(begins(0, [0]), attended, out_weight, share, after)
        if cores > 1:
            mine = mine + to_core(send).astype(jnp.float32)
    else:
        mine = products[1]
        if cores > 1:
            mine = mine + to_core(products[0]).astype(jnp.float32)
    result = []
    for cut, found in enumerate(arriving):
        total = mine[:, cuts[cut] : cuts[cut + 1]]
        for x in found:
            total = total + x.astype(jnp.float32)
        result.append(total.astype(jnp.bfloat16))
    return jnp.concatenate(result, axis=1)


def solution(mesh):
    in_specs = (P("ctx", "tp"), P("ctx", None), P("ctx", None), P("tp", None), P("ctx"))
    out_specs = P("ctx", "tp")

    def layer(*args):
        return shards(mesh.shape["ctx"], mesh.shape["tp"], *args)

    return jax.shard_map(
        layer, mesh=mesh, in_specs=in_specs, out_specs=out_specs, check_vma=False
    )
```

```python
import functools
import math

import jax
import jax.numpy as jnp
from jax import lax
from jax.experimental import pallas as pl
from jax.experimental.pallas import tpu as pltpu
from jax.sharding import PartitionSpec as P

QUERY_HEADS = 64
KEY_VALUE_HEADS = 8
HEAD_SIZE = 128
HIDDEN = -1e30
TAIL = 16
DIGIT = 128
WHOLE = pl.BlockSpec(memory_space=pltpu.VMEM)
NT = (((1,), (1,)), ((), ()))
DEPTH = 4
VMEM_LIMIT = 16 << 20
WIDE_LIMIT = 48 << 20


def fetch_columns(at_ref, weight_ref, buffer, sem, counts, started=None):
    wide = buffer.shape[2]
    copies = []
    for run, count in enumerate(counts):
        for tile in range(count):
            column = pl.multiple_of(at_ref[run] + tile * wide, wide)
            n = len(copies)
            copies.append(
                pltpu.make_async_copy(
                    weight_ref.at[:, pl.ds(column, wide)], buffer.at[n], sem.at[n]
                )
            )
    for copy in copies[:started]:
        copy.start()
    return copies


def multiply_columns(rows_ref, buffer, copies, outs):
    wide = buffer.shape[2]
    n = 0
    for out in outs:
        for tile in range(out.shape[1] // wide):
            if copies is not None:
                copies[n].wait()
                if n + DEPTH < len(copies):
                    copies[n + DEPTH].start()
            out[:, tile * wide : (tile + 1) * wide] = jnp.dot(
                rows_ref[...], buffer[n], preferred_element_type=jnp.float32
            ).astype(out.dtype)
            n += 1


def attend_kernel(halves, first, last, scale, kv_heads, span, *refs):
    n_blocks = len(halves)
    order_ref, q_ref = refs[:2]
    blocks, refs = [], refs[2:]
    for count in halves:
        blocks.append(refs[:count])
        refs = refs[count:]
    if not first:
        old_top, old_total, old_acc = refs[:3]
        refs = refs[3:]
    if last:
        at_ref, weight_ref = refs[:2]
        buffer, sem = refs[-2:]
        refs = refs[2:-2]
        products = refs[1:-7]
        counts = [out.shape[1] // buffer.shape[2] for out in products]
        copies = fetch_columns(at_ref, weight_ref, buffer, sem, counts)
    outs = refs[:3]
    merged_ref, bias_ref, flip_ref = refs[-7:-4]
    score_refs, weight_refs = refs[-4:-2], refs[-2:]
    parts = order_ref.shape[0]
    rows = q_ref.shape[0] // parts
    heads = q_ref.shape[1] // kv_heads // HEAD_SIZE
    pair = span // rows
    for b, found in enumerate(blocks):
        if len(found) == 2:
            merged_ref[b] = found[0][...] + found[1][...]
            blocks[b] = merged_ref.at[b]
        else:
            blocks[b] = found[0]
    lengths = [block.shape[0] - TAIL for block in blocks]
    offsets = [sum(lengths[:b]) for b in range(n_blocks)]

    key_at = lax.broadcasted_iota(jnp.int32, (rows, rows), 0).astype(jnp.float32)
    query_iota = lax.broadcasted_iota(jnp.int32, (rows, rows), 1)
    for block, length, offset in zip(blocks, lengths, offsets):
        tail = block[length : length + TAIL, 0:HEAD_SIZE].astype(jnp.float32)
        for part in range(length // rows):
            high, low = tail[2 * part : 2 * part + 1, :], tail[2 * part + 1 : 2 * part + 2, :]
            key_pos = (high * DIGIT + low)[:, 0:rows] * float(rows) + key_at
            at = slice(offset + part * rows, offset + (part + 1) * rows)
            for i in range(parts):
                query_pos = (query_iota + order_ref[i] * rows).astype(jnp.float32)
                bias_ref[i, at, :] = jnp.where(key_pos > query_pos, HIDDEN, 0.0)
        for k in range(kv_heads):
            at = slice((2 * k + 1) * HEAD_SIZE, (2 * k + 2) * HEAD_SIZE)
            flip_ref[k, :, offset : offset + length] = block[0:length, at].T

    pieces = [
        (k, i, p) for k in range(kv_heads) for i in range(parts) for p in range(heads // pair)
    ]
    tops, totals = {}, {}

    def head_cols(k, p, j):
        head = k * heads + p * pair + j
        return slice(head * HEAD_SIZE, (head + 1) * HEAD_SIZE)

    def score(t):
        k, i, p = pieces[t]
        q = jnp.concatenate(
            [q_ref[i * rows : (i + 1) * rows, head_cols(k, p, j)] for j in range(pair)], axis=0
        )
        top = None
        for block, length, offset in zip(blocks, lengths, offsets):
            key = block[0:length, 2 * k * HEAD_SIZE : (2 * k + 1) * HEAD_SIZE]
            tile = bias_ref[i, offset : offset + length, :]
            scores = lax.dot_general(key, q, NT, preferred_element_type=jnp.float32)
            scores = scores * scale + jnp.concatenate([tile] * pair, axis=1)
            score_refs[t % 2][offset : offset + length, :] = scores
            part = jnp.max(scores, axis=0, keepdims=True)
            top = part if top is None else jnp.maximum(top, part)
        if not first:
            top = jnp.maximum(top, old_top[k * parts + i, :, p * span : (p + 1) * span])
        tops[t] = top

    def weigh(t):
        weights = jnp.exp2(score_refs[t % 2][...] - tops[t])
        totals[t] = jnp.sum(weights, axis=0, keepdims=True)
        weight_refs[t % 2][...] = weights.astype(jnp.bfloat16)

    def spread(t):
        k, i, p = pieces[t]
        at = slice(p * span, (p + 1) * span)
        c = k * parts + i
        acc = jnp.dot(flip_ref[k], weight_refs[t % 2][...], preferred_element_type=jnp.float32)
        total = totals[t]
        if not first:
            factor = jnp.exp2(old_top[c, :, at] - tops[t])
            total = total + old_total[c, :, at] * factor
            acc = acc + old_acc[c, :, at] * factor
        if last:
            done = (acc * (1.0 / total)).T.astype(jnp.bfloat16)
            for j in range(pair):
                outs[0][i * rows : (i + 1) * rows, head_cols(k, p, j)] = done[
                    j * rows : (j + 1) * rows, :
                ]
        else:
            outs[0][c, :, at] = tops[t]
            outs[1][c, :, at] = total
            outs[2][c, :, at] = acc

    for t in range(len(pieces) + 2):
        if t < len(pieces):
            score(t)
        if t >= 2:
            spread(t - 2)
        if 1 <= t <= len(pieces):
            weigh(t - 1)
    if last:
        for copy in copies:
            copy.wait()
        multiply_columns(outs[0], buffer, None, products)


def product_shapes(tokens, widths):
    found = []
    for width in widths:
        found.append(jax.ShapeDtypeStruct((tokens, width), jnp.bfloat16))
        found.append(jax.ShapeDtypeStruct((tokens, width), jnp.float32))
    return found


def column_scratch(depth, widths):
    wide = math.gcd(512, *widths)
    tiles = 2 * sum(widths) // wide
    return [pltpu.VMEM((tiles, depth, wide), jnp.bfloat16), pltpu.SemaphoreType.DMA((tiles,))]


def attend(order, queries, blocks, state, kv_heads, then=None):
    tokens, width = queries.shape
    parts = order.shape[0]
    rows = tokens // parts
    heads = width // kv_heads // HEAD_SIZE
    span = math.gcd(heads, 2) * rows
    scale = math.log2(math.e) / math.sqrt(HEAD_SIZE)
    first, last = state is None, then is not None
    seen = sum(block[0].shape[0] - TAIL for block in blocks)
    pairs = tokens * width // HEAD_SIZE * seen
    whole = pl.BlockSpec(memory_space=pltpu.VMEM)
    scalars = pl.BlockSpec(memory_space=pltpu.SMEM)
    combos = kv_heads * parts
    halves = [len(block) for block in blocks]
    arrays = [array for block in blocks for array in block]
    operands = [order, queries, *arrays, *(() if first else state)]
    in_specs = [scalars] + [whole] * (len(operands) - 1)
    scratch = [
        pltpu.VMEM((len(blocks), *arrays[0].shape), arrays[0].dtype),
        pltpu.VMEM((parts, seen, rows), jnp.float32),
        pltpu.VMEM((kv_heads, HEAD_SIZE, seen), jnp.bfloat16),
    ]
    scratch += [pltpu.VMEM((seen, span), jnp.float32)] * 2
    scratch += [pltpu.VMEM((seen, span), jnp.bfloat16)] * 2
    flops = 4 * pairs * HEAD_SIZE
    if last:
        at, weight, widths = then
        operands += [at, weight]
        in_specs += [scalars, pl.BlockSpec(memory_space=pl.ANY)]
        out_shape = [jax.ShapeDtypeStruct(queries.shape, jnp.bfloat16)]
        out_shape += product_shapes(tokens, widths)
        scratch += column_scratch(width, widths)
        flops += 4 * tokens * width * sum(widths)
    else:
        out_shape = [
            jax.ShapeDtypeStruct((combos, 1, heads * rows), jnp.float32),
            jax.ShapeDtypeStruct((combos, 1, heads * rows), jnp.float32),
            jax.ShapeDtypeStruct((combos, HEAD_SIZE, heads * rows), jnp.float32),
        ]
    return pl.pallas_call(
        functools.partial(attend_kernel, halves, first, last, scale, kv_heads, span),
        in_specs=in_specs,
        out_specs=[whole] * len(out_shape),
        out_shape=out_shape,
        scratch_shapes=scratch,
        compiler_params=pltpu.CompilerParams(vmem_limit_bytes=WIDE_LIMIT if last else VMEM_LIMIT),
        cost_estimate=pl.CostEstimate(
            flops=flops, bytes_accessed=4 * pairs, transcendentals=pairs
        ),
    )(*operands)


def project_kernel(at_ref, rows_ref, weight_ref, *refs):
    send_ref, keep_ref, buffer, sem = refs[-4:]
    counts = [out.shape[1] // buffer.shape[2] for out in (send_ref, keep_ref)]
    copies = fetch_columns(at_ref, weight_ref, buffer, sem, counts, DEPTH)
    multiply_columns(rows_ref, buffer, copies, (send_ref, keep_ref))


def project(at, attended, weight, columns, after):
    tokens, depth = attended.shape
    whole = pl.BlockSpec(memory_space=pltpu.VMEM)
    unread = pl.BlockSpec(memory_space=pl.ANY)
    return pl.pallas_call(
        project_kernel,
        in_specs=[pl.BlockSpec(memory_space=pltpu.SMEM), whole, unread] + [unread] * len(after),
        out_specs=[whole] * 2,
        out_shape=product_shapes(tokens, [columns]),
        scratch_shapes=column_scratch(depth, [columns]),
        compiler_params=pltpu.CompilerParams(vmem_limit_bytes=WIDE_LIMIT),
        cost_estimate=pl.CostEstimate(
            flops=4 * tokens * depth * columns,
            bytes_accessed=4 * depth * columns,
            transcendentals=0,
        ),
    )(at, attended, weight, *after)


def add_up_kernel(cuts, n_swapped, mine_ref, *refs):
    out_ref = refs[-1]
    swapped, arrived = refs[:n_swapped], refs[n_swapped:-1]
    each = len(arrived) // (len(cuts) - 1)
    for cut in range(len(cuts) - 1):
        at = slice(cuts[cut], cuts[cut + 1])
        total = mine_ref[:, at]
        for ref in swapped:
            total = total + ref[:, at].astype(jnp.float32)
        for ref in arrived[cut * each : (cut + 1) * each]:
            total = total + ref[...].astype(jnp.float32)
        out_ref[:, at] = total.astype(out_ref.dtype)


def add_up(mine, swapped, arriving, cuts):
    arrived = [x for found in arriving for x in found]
    return pl.pallas_call(
        functools.partial(add_up_kernel, cuts, len(swapped)),
        in_specs=[WHOLE] * (1 + len(swapped) + len(arrived)),
        out_specs=WHOLE,
        out_shape=jax.ShapeDtypeStruct(mine.shape, jnp.bfloat16),
        compiler_params=pltpu.CompilerParams(vmem_limit_bytes=VMEM_LIMIT),
        cost_estimate=pl.CostEstimate(
            flops=4 * mine.size, bytes_accessed=10 * mine.size, transcendentals=0
        ),
    )(mine, *swapped, *arrived)


def shards(n_ctx, n_tp, queries, keys, values, out_weight, block_order):
    heads_dev = queries.shape[1] // HEAD_SIZE
    group_size = QUERY_HEADS // KEY_VALUE_HEADS
    kv_heads = max(1, heads_dev // group_size)
    tp = lax.axis_index("tp")
    start = tp * heads_dev // group_size * HEAD_SIZE
    own_keys = lax.dynamic_slice_in_dim(keys, start, kv_heads * HEAD_SIZE, 1)
    own_values = lax.dynamic_slice_in_dim(values, start, kv_heads * HEAD_SIZE, 1)
    pieces = []
    for head in range(kv_heads):
        at = slice(head * HEAD_SIZE, (head + 1) * HEAD_SIZE)
        pieces += [own_keys[:, at], own_values[:, at]]
    body = jnp.concatenate(pieces, axis=1)
    digits = jnp.stack([block_order // DIGIT, block_order % DIGIT], axis=1).reshape(-1)
    digits = jnp.pad(digits, (0, TAIL - digits.shape[0])).astype(jnp.bfloat16)
    tail = jnp.broadcast_to(digits[:, None], (TAIL, body.shape[1]))
    own = jnp.concatenate([body, tail], axis=0)

    inner = math.gcd(n_ctx, 2)
    outer = n_ctx // inner

    def move(block, target):
        pairs = []
        for o in range(outer):
            for i in range(inner):
                to = target(o, i)
                if to is not None:
                    pairs.append((o * inner + i, to[0] * inner + to[1]))
        return lax.ppermute(block, "ctx", pairs)

    def cross(block, among=None):
        found = []
        for k in range(1, inner):

            def target(o, i):
                return (o, (i + k) % inner) if among is None or o in among else None

            found.append(move(block, target))
        return found

    if outer == 4:
        near = move(own, lambda o, i: (o ^ 1, i))
        own_crossed = cross(own)
        mid = move(own, lambda o, i: {1: (2, i), 2: (1, i)}.get(o))
        far = move(own, lambda o, i: {0: (3, i), 3: (0, i)}.get(o))
        third = move(own, lambda o, i: {0: (2, i), 3: (1, i)}.get(o))
        near_crossed = cross(near)
        onward = move(mid, lambda o, i: {2: (3, i), 1: (0, i)}.get(o))
        middle, ends = (1, 2), (0, 3)
        stages = [[(own,), (near,)] + [(x,) for x in own_crossed]]
        stages.append([(mid, far)] + [(x,) for x in near_crossed] + [(third, onward)])
        for a, b in ((mid, far), (third, onward)):
            crossed = zip(cross(a, middle), cross(b, ends))
            stages += [[pair] for pair in crossed]
    else:
        blocks = [own]
        for k in range(1, outer):
            blocks.append(move(own, lambda o, i: ((o + k) % outer, i)))
        arrived = blocks[1:]
        for k, block in enumerate(blocks):
            arrived += cross(block)
        arrived = [(x,) for x in arrived]
        stages = [[(own,)]]
        stages += [arrived[i : min(i + 3, len(arrived) - 1)] for i in range(0, len(arrived) - 1, 3)]
        stages += [arrived[-1:]] if arrived else []

    share = out_weight.shape[1] // n_tp
    cores = math.gcd(n_tp, 2)
    groups = n_tp // cores
    core, group = tp % cores, tp // cores
    cuts = [0, share // 4, share] if groups == 2 else [0, share]
    widths = [b - a for a, b in zip(cuts, cuts[1:])]
    jobs = [(cut, r) for r in range(1, groups) for cut in range(len(widths))]

    def begins(r, numbers):
        to = (group + r) % groups * cores
        firsts = jnp.stack([to + (core + 1) % cores, to + core]) * share
        return jnp.concatenate([firsts + cuts[n] for n in numbers]).astype(jnp.int32)

    def to_core(x):
        pairs = [(t, t // cores * cores + (t + 1) % cores) for t in range(n_tp)]
        return lax.ppermute(x, "tp", pairs)

    def to_group(x, r):
        pairs = [(t, (t + r * cores) % n_tp) for t in range(n_tp)]
        return lax.ppermute(x, "tp", pairs)

    state = None
    for blocks in stages[:-1]:
        state = attend(block_order, queries, blocks, state, kv_heads)
    together = list(range(len(widths)))
    attended, *products = attend(
        block_order,
        queries,
        stages[-1],
        state,
        kv_heads,
        (begins(min(1, groups - 1), together), out_weight, widths),
    )
    for r in range(2, groups):
        for cut in together:
            products += project(
                begins(r, [cut]), attended, out_weight, widths[cut], products[-2:-1]
            )

    arriving = [[] for _ in widths]
    after = ()
    others = [to_core(products[2 * n]) for n in range(len(jobs))] if cores > 1 else None
    for name, (cut, r) in enumerate(jobs):
        total = products[2 * name + 1]
        if cores > 1:
            total = total + others[name].astype(jnp.float32)
        total = total.astype(jnp.bfloat16)
        after += (total,)
        arriving[cut].append(to_group(total, r))
    if jobs:
        send, mine = project(begins(0, [0]), attended, out_weight, share, after)
    else:
        send, mine = products
    swapped = [to_core(send)] if cores > 1 else []
    return add_up(mine, swapped, arriving, cuts)


def solution(mesh):
    in_specs = (P("ctx", "tp"), P("ctx", None), P("ctx", None), P("tp", None), P("ctx"))
    out_specs = P("ctx", "tp")

    def layer(*args):
        return shards(mesh.shape["ctx"], mesh.shape["tp"], *args)

    return jax.shard_map(
        layer, mesh=mesh, in_specs=in_specs, out_specs=out_specs, check_vma=False
    )
```

```python
import functools
import math

import jax
import jax.numpy as jnp
from jax import lax
from jax.experimental import pallas as pl
from jax.experimental.pallas import tpu as pltpu
from jax.sharding import PartitionSpec as P

QUERY_HEADS = 64
KEY_VALUE_HEADS = 8
HEAD_SIZE = 128
HIDDEN = -1e30
TAIL = 16
DIGIT = 128
WHOLE = pl.BlockSpec(memory_space=pltpu.VMEM)
NT = (((1,), (1,)), ((), ()))
DEPTH = 4
VMEM_LIMIT = 16 << 20
WIDE_LIMIT = 48 << 20


def fetch_columns(at_ref, weight_ref, buffer, sem, counts, started=None):
    wide = buffer.shape[2]
    copies = []
    for run, count in enumerate(counts):
        for tile in range(count):
            column = pl.multiple_of(at_ref[run] + tile * wide, wide)
            n = len(copies)
            copies.append(
                pltpu.make_async_copy(
                    weight_ref.at[:, pl.ds(column, wide)], buffer.at[n], sem.at[n]
                )
            )
    for copy in copies[:started]:
        copy.start()
    return copies


def multiply_columns(rows_ref, buffer, copies, outs):
    wide = buffer.shape[2]
    n = 0
    for out in outs:
        for tile in range(out.shape[1] // wide):
            if copies is not None:
                copies[n].wait()
                if n + DEPTH < len(copies):
                    copies[n + DEPTH].start()
            out[:, tile * wide : (tile + 1) * wide] = jnp.dot(
                rows_ref[...], buffer[n], preferred_element_type=jnp.float32
            ).astype(out.dtype)
            n += 1


def attend_kernel(halves, first, last, scale, kv_heads, span, *refs):
    n_blocks = len(halves)
    order_ref, q_ref = refs[:2]
    blocks, refs = [], refs[2:]
    for count in halves:
        blocks.append(refs[:count])
        refs = refs[count:]
    if not first:
        old_top, old_total, old_acc = refs[:3]
        refs = refs[3:]
    if last:
        at_ref, weight_ref = refs[:2]
        buffer, sem = refs[-2:]
        refs = refs[2:-2]
        products = refs[1:-7]
        counts = [out.shape[1] // buffer.shape[2] for out in products]
        copies = fetch_columns(at_ref, weight_ref, buffer, sem, counts)
    outs = refs[:3]
    merged_ref, bias_ref, flip_ref = refs[-7:-4]
    score_refs, weight_refs = refs[-4:-2], refs[-2:]
    parts = order_ref.shape[0]
    rows = q_ref.shape[0] // parts
    heads = q_ref.shape[1] // kv_heads // HEAD_SIZE
    pair = span // rows
    for b, found in enumerate(blocks):
        if len(found) == 2:
            merged_ref[b] = found[0][...] + found[1][...]
            blocks[b] = merged_ref.at[b]
        else:
            blocks[b] = found[0]
    lengths = [block.shape[0] - TAIL for block in blocks]
    offsets = [sum(lengths[:b]) for b in range(n_blocks)]

    key_at = lax.broadcasted_iota(jnp.int32, (rows, rows), 0).astype(jnp.float32)
    query_iota = lax.broadcasted_iota(jnp.int32, (rows, rows), 1)
    for block, length, offset in zip(blocks, lengths, offsets):
        tail = block[length : length + TAIL, 0:HEAD_SIZE].astype(jnp.float32)
        for part in range(length // rows):
            high, low = tail[2 * part : 2 * part + 1, :], tail[2 * part + 1 : 2 * part + 2, :]
            key_pos = (high * DIGIT + low)[:, 0:rows] * float(rows) + key_at
            at = slice(offset + part * rows, offset + (part + 1) * rows)
            for i in range(parts):
                query_pos = (query_iota + order_ref[i] * rows).astype(jnp.float32)
                bias_ref[i, at, :] = jnp.where(key_pos > query_pos, HIDDEN, 0.0)
        for k in range(kv_heads):
            at = slice((2 * k + 1) * HEAD_SIZE, (2 * k + 2) * HEAD_SIZE)
            flip_ref[k, :, offset : offset + length] = block[0:length, at].T

    pieces = [
        (k, i, p) for k in range(kv_heads) for i in range(parts) for p in range(heads // pair)
    ]
    tops, totals = {}, {}

    def head_cols(k, p, j):
        head = k * heads + p * pair + j
        return slice(head * HEAD_SIZE, (head + 1) * HEAD_SIZE)

    def score(t):
        k, i, p = pieces[t]
        q = jnp.concatenate(
            [q_ref[i * rows : (i + 1) * rows, head_cols(k, p, j)] for j in range(pair)], axis=0
        )
        top = None
        for block, length, offset in zip(blocks, lengths, offsets):
            key = block[0:length, 2 * k * HEAD_SIZE : (2 * k + 1) * HEAD_SIZE]
            tile = bias_ref[i, offset : offset + length, :]
            scores = lax.dot_general(key, q, NT, preferred_element_type=jnp.float32)
            scores = scores * scale + jnp.concatenate([tile] * pair, axis=1)
            score_refs[t % 2][offset : offset + length, :] = scores
            part = jnp.max(scores, axis=0, keepdims=True)
            top = part if top is None else jnp.maximum(top, part)
        if not first:
            top = jnp.maximum(top, old_top[k * parts + i, :, p * span : (p + 1) * span])
        tops[t] = top

    def weigh(t):
        weights = jnp.exp2(score_refs[t % 2][...] - tops[t])
        totals[t] = jnp.sum(weights, axis=0, keepdims=True)
        weight_refs[t % 2][...] = weights.astype(jnp.bfloat16)

    def spread(t):
        k, i, p = pieces[t]
        at = slice(p * span, (p + 1) * span)
        c = k * parts + i
        acc = jnp.dot(flip_ref[k], weight_refs[t % 2][...], preferred_element_type=jnp.float32)
        total = totals[t]
        if not first:
            factor = jnp.exp2(old_top[c, :, at] - tops[t])
            total = total + old_total[c, :, at] * factor
            acc = acc + old_acc[c, :, at] * factor
        if last:
            done = (acc * (1.0 / total)).T.astype(jnp.bfloat16)
            for j in range(pair):
                outs[0][i * rows : (i + 1) * rows, head_cols(k, p, j)] = done[
                    j * rows : (j + 1) * rows, :
                ]
        else:
            outs[0][c, :, at] = tops[t]
            outs[1][c, :, at] = total
            outs[2][c, :, at] = acc

    for t in range(len(pieces) + 2):
        if t < len(pieces):
            score(t)
        if t >= 2:
            spread(t - 2)
        if 1 <= t <= len(pieces):
            weigh(t - 1)
    if last:
        for copy in copies:
            copy.wait()
        multiply_columns(outs[0], buffer, None, products)


def product_shapes(tokens, widths):
    found = []
    for width in widths:
        found.append(jax.ShapeDtypeStruct((tokens, width), jnp.bfloat16))
        found.append(jax.ShapeDtypeStruct((tokens, width), jnp.float32))
    return found


def column_scratch(depth, widths):
    wide = math.gcd(512, *widths)
    tiles = 2 * sum(widths) // wide
    return [pltpu.VMEM((tiles, depth, wide), jnp.bfloat16), pltpu.SemaphoreType.DMA((tiles,))]


def attend(order, queries, blocks, state, kv_heads, then=None):
    tokens, width = queries.shape
    parts = order.shape[0]
    rows = tokens // parts
    heads = width // kv_heads // HEAD_SIZE
    span = math.gcd(heads, 2) * rows
    scale = math.log2(math.e) / math.sqrt(HEAD_SIZE)
    first, last = state is None, then is not None
    seen = sum(block[0].shape[0] - TAIL for block in blocks)
    pairs = tokens * width // HEAD_SIZE * seen
    whole = pl.BlockSpec(memory_space=pltpu.VMEM)
    scalars = pl.BlockSpec(memory_space=pltpu.SMEM)
    combos = kv_heads * parts
    halves = [len(block) for block in blocks]
    arrays = [array for block in blocks for array in block]
    operands = [order, queries, *arrays, *(() if first else state)]
    in_specs = [scalars] + [whole] * (len(operands) - 1)
    scratch = [
        pltpu.VMEM((len(blocks), *arrays[0].shape), arrays[0].dtype),
        pltpu.VMEM((parts, seen, rows), jnp.float32),
        pltpu.VMEM((kv_heads, HEAD_SIZE, seen), jnp.bfloat16),
    ]
    scratch += [pltpu.VMEM((seen, span), jnp.float32)] * 2
    scratch += [pltpu.VMEM((seen, span), jnp.bfloat16)] * 2
    flops = 4 * pairs * HEAD_SIZE
    if last:
        at, weight, widths = then
        operands += [at, weight]
        in_specs += [scalars, pl.BlockSpec(memory_space=pl.ANY)]
        out_shape = [jax.ShapeDtypeStruct(queries.shape, jnp.bfloat16)]
        out_shape += product_shapes(tokens, widths)
        scratch += column_scratch(width, widths)
        flops += 4 * tokens * width * sum(widths)
    else:
        out_shape = [
            jax.ShapeDtypeStruct((combos, 1, heads * rows), jnp.float32),
            jax.ShapeDtypeStruct((combos, 1, heads * rows), jnp.float32),
            jax.ShapeDtypeStruct((combos, HEAD_SIZE, heads * rows), jnp.float32),
        ]
    return pl.pallas_call(
        functools.partial(attend_kernel, halves, first, last, scale, kv_heads, span),
        in_specs=in_specs,
        out_specs=[whole] * len(out_shape),
        out_shape=out_shape,
        scratch_shapes=scratch,
        compiler_params=pltpu.CompilerParams(vmem_limit_bytes=WIDE_LIMIT if last else VMEM_LIMIT),
        cost_estimate=pl.CostEstimate(
            flops=flops, bytes_accessed=4 * pairs, transcendentals=pairs
        ),
    )(*operands)


def project_kernel(at_ref, rows_ref, weight_ref, *refs):
    send_ref, keep_ref, buffer, sem = refs[-4:]
    counts = [out.shape[1] // buffer.shape[2] for out in (send_ref, keep_ref)]
    copies = fetch_columns(at_ref, weight_ref, buffer, sem, counts, DEPTH)
    multiply_columns(rows_ref, buffer, copies, (send_ref, keep_ref))


def project(at, attended, weight, columns, after):
    tokens, depth = attended.shape
    whole = pl.BlockSpec(memory_space=pltpu.VMEM)
    unread = pl.BlockSpec(memory_space=pl.ANY)
    return pl.pallas_call(
        project_kernel,
        in_specs=[pl.BlockSpec(memory_space=pltpu.SMEM), whole, unread] + [unread] * len(after),
        out_specs=[whole] * 2,
        out_shape=product_shapes(tokens, [columns]),
        scratch_shapes=column_scratch(depth, [columns]),
        compiler_params=pltpu.CompilerParams(vmem_limit_bytes=WIDE_LIMIT),
        cost_estimate=pl.CostEstimate(
            flops=4 * tokens * depth * columns,
            bytes_accessed=4 * depth * columns,
            transcendentals=0,
        ),
    )(at, attended, weight, *after)


def add_up_kernel(cuts, n_swapped, mine_ref, *refs):
    out_ref = refs[-1]
    swapped, arrived = refs[:n_swapped], refs[n_swapped:-1]
    each = len(arrived) // (len(cuts) - 1)
    for cut in range(len(cuts) - 1):
        at = slice(cuts[cut], cuts[cut + 1])
        total = mine_ref[:, at]
        for ref in swapped:
            total = total + ref[:, at].astype(jnp.float32)
        for ref in arrived[cut * each : (cut + 1) * each]:
            total = total + ref[...].astype(jnp.float32)
        out_ref[:, at] = total.astype(out_ref.dtype)


def add_up(mine, swapped, arriving, cuts):
    arrived = [x for found in arriving for x in found]
    return pl.pallas_call(
        functools.partial(add_up_kernel, cuts, len(swapped)),
        in_specs=[WHOLE] * (1 + len(swapped) + len(arrived)),
        out_specs=WHOLE,
        out_shape=jax.ShapeDtypeStruct(mine.shape, jnp.bfloat16),
        compiler_params=pltpu.CompilerParams(vmem_limit_bytes=VMEM_LIMIT),
        cost_estimate=pl.CostEstimate(
            flops=4 * mine.size, bytes_accessed=10 * mine.size, transcendentals=0
        ),
    )(mine, *swapped, *arrived)


def shards(n_ctx, n_tp, queries, keys, values, out_weight, block_order):
    heads_dev = queries.shape[1] // HEAD_SIZE
    group_size = QUERY_HEADS // KEY_VALUE_HEADS
    kv_heads = max(1, heads_dev // group_size)
    tp = lax.axis_index("tp")
    start = tp * heads_dev // group_size * HEAD_SIZE
    own_keys = lax.dynamic_slice_in_dim(keys, start, kv_heads * HEAD_SIZE, 1)
    own_values = lax.dynamic_slice_in_dim(values, start, kv_heads * HEAD_SIZE, 1)
    pieces = []
    for head in range(kv_heads):
        at = slice(head * HEAD_SIZE, (head + 1) * HEAD_SIZE)
        pieces += [own_keys[:, at], own_values[:, at]]
    body = jnp.concatenate(pieces, axis=1)
    digits = jnp.stack([block_order // DIGIT, block_order % DIGIT], axis=1).reshape(-1)
    digits = jnp.pad(digits, (0, TAIL - digits.shape[0])).astype(jnp.bfloat16)
    tail = jnp.broadcast_to(digits[:, None], (TAIL, body.shape[1]))
    own = jnp.concatenate([body, tail], axis=0)

    inner = math.gcd(n_ctx, 2)
    outer = n_ctx // inner

    def move(block, target):
        pairs = []
        for o in range(outer):
            for i in range(inner):
                to = target(o, i)
                if to is not None:
                    pairs.append((o * inner + i, to[0] * inner + to[1]))
        return lax.ppermute(block, "ctx", pairs)

    def cross(block, among=None):
        found = []
        for k in range(1, inner):

            def target(o, i):
                return (o, (i + k) % inner) if among is None or o in among else None

            found.append(move(block, target))
        return found

    if outer == 4:
        near = move(own, lambda o, i: (o ^ 1, i))
        mid = move(own, lambda o, i: {1: (2, i), 2: (1, i)}.get(o))
        own_crossed = cross(own)
        onward = move(mid, lambda o, i: {2: (3, i), 1: (0, i)}.get(o))
        third = move(own, lambda o, i: {0: (2, i), 3: (1, i)}.get(o))
        near_crossed = cross(near)
        mid_crossed = cross(mid, (1, 2))
        far = move(own, lambda o, i: {0: (3, i), 3: (0, i)}.get(o))
        third_crossed = list(zip(cross(third, (1, 2)), cross(onward, (0, 3))))
        far_crossed = cross(far, (0, 3))
        stages = [[(own,), (near,)] + [(x,) for x in own_crossed]]
        stages.append([(third, onward)] + [(x,) for x in near_crossed])
        stages.append([(mid, far)] + third_crossed)
        stages += [[pair] for pair in zip(mid_crossed, far_crossed)]
    else:
        blocks = [own]
        for k in range(1, outer):
            blocks.append(move(own, lambda o, i: ((o + k) % outer, i)))
        arrived = blocks[1:]
        for k, block in enumerate(blocks):
            arrived += cross(block)
        arrived = [(x,) for x in arrived]
        stages = [[(own,)]]
        stages += [arrived[i : min(i + 3, len(arrived) - 1)] for i in range(0, len(arrived) - 1, 3)]
        stages += [arrived[-1:]] if arrived else []

    share = out_weight.shape[1] // n_tp
    cores = math.gcd(n_tp, 2)
    groups = n_tp // cores
    core, group = tp % cores, tp // cores
    cuts = [0, share // 4, share] if groups == 2 else [0, share]
    widths = [b - a for a, b in zip(cuts, cuts[1:])]
    jobs = [(cut, r) for r in range(1, groups) for cut in range(len(widths))]

    def begins(r, numbers):
        to = (group + r) % groups * cores
        firsts = jnp.stack([to + (core + 1) % cores, to + core]) * share
        return jnp.concatenate([firsts + cuts[n] for n in numbers]).astype(jnp.int32)

    def to_core(x):
        pairs = [(t, t // cores * cores + (t + 1) % cores) for t in range(n_tp)]
        return lax.ppermute(x, "tp", pairs)

    def to_group(x, r):
        pairs = [(t, (t + r * cores) % n_tp) for t in range(n_tp)]
        return lax.ppermute(x, "tp", pairs)

    state = None
    for blocks in stages[:-1]:
        state = attend(block_order, queries, blocks, state, kv_heads)
    together = list(range(len(widths)))
    attended, *products = attend(
        block_order,
        queries,
        stages[-1],
        state,
        kv_heads,
        (begins(min(1, groups - 1), together), out_weight, widths),
    )
    for r in range(2, groups):
        for cut in together:
            products += project(
                begins(r, [cut]), attended, out_weight, widths[cut], products[-2:-1]
            )

    arriving = [[] for _ in widths]
    after = ()
    others = [to_core(products[2 * n]) for n in range(len(jobs))] if cores > 1 else None
    for name, (cut, r) in enumerate(jobs):
        total = products[2 * name + 1]
        if cores > 1:
            total = total + others[name].astype(jnp.float32)
        total = total.astype(jnp.bfloat16)
        after += (total,)
        arriving[cut].append(to_group(total, r))
    if jobs:
        send, mine = project(begins(0, [0]), attended, out_weight, share, after)
    else:
        send, mine = products
    swapped = [to_core(send)] if cores > 1 else []
    return add_up(mine, swapped, arriving, cuts)


def solution(mesh):
    in_specs = (P("ctx", "tp"), P("ctx", None), P("ctx", None), P("tp", None), P("ctx"))
    out_specs = P("ctx", "tp")

    def layer(*args):
        return shards(mesh.shape["ctx"], mesh.shape["tp"], *args)

    return jax.shard_map(
        layer, mesh=mesh, in_specs=in_specs, out_specs=out_specs, check_vma=False
    )
```

```python
import functools
import math

import jax
import jax.numpy as jnp
from jax import lax
from jax.experimental import pallas as pl
from jax.experimental.pallas import tpu as pltpu
from jax.sharding import PartitionSpec as P

QUERY_HEADS = 64
KEY_VALUE_HEADS = 8
HEAD_SIZE = 128
HIDDEN = -1e30
TAIL = 16
DIGIT = 128
WHOLE = pl.BlockSpec(memory_space=pltpu.VMEM)
NT = (((1,), (1,)), ((), ()))
DEPTH = 4
VMEM_LIMIT = 16 << 20
WIDE_LIMIT = 48 << 20


def fetch_columns(at_ref, weight_ref, buffer, sem, counts, started=None):
    wide = buffer.shape[2]
    copies = []
    for run, count in enumerate(counts):
        for tile in range(count):
            column = pl.multiple_of(at_ref[run] + tile * wide, wide)
            n = len(copies)
            copies.append(
                pltpu.make_async_copy(
                    weight_ref.at[:, pl.ds(column, wide)], buffer.at[n], sem.at[n]
                )
            )
    for copy in copies[:started]:
        copy.start()
    return copies


def multiply_columns(rows_ref, buffer, copies, outs):
    wide = buffer.shape[2]
    n = 0
    for out in outs:
        for tile in range(out.shape[1] // wide):
            if copies is not None:
                copies[n].wait()
                if n + DEPTH < len(copies):
                    copies[n + DEPTH].start()
            out[:, tile * wide : (tile + 1) * wide] = jnp.dot(
                rows_ref[...], buffer[n], preferred_element_type=jnp.float32
            ).astype(out.dtype)
            n += 1


def attend_kernel(halves, first, last, scale, kv_heads, span, *refs):
    n_blocks = len(halves)
    order_ref, q_ref = refs[:2]
    blocks, refs = [], refs[2:]
    for count in halves:
        blocks.append(refs[:count])
        refs = refs[count:]
    if not first:
        old_top, old_total, old_acc = refs[:3]
        refs = refs[3:]
    if last:
        at_ref, weight_ref = refs[:2]
        buffer, sem = refs[-2:]
        refs = refs[2:-2]
        products = refs[1:-7]
        counts = [out.shape[1] // buffer.shape[2] for out in products]
        copies = fetch_columns(at_ref, weight_ref, buffer, sem, counts)
    outs = refs[:3]
    merged_ref, bias_ref, flip_ref = refs[-7:-4]
    score_refs, weight_refs = refs[-4:-2], refs[-2:]
    parts = order_ref.shape[0]
    rows = q_ref.shape[0] // parts
    heads = q_ref.shape[1] // kv_heads // HEAD_SIZE
    pair = span // rows
    for b, found in enumerate(blocks):
        if len(found) == 2:
            merged_ref[b] = found[0][...] + found[1][...]
            blocks[b] = merged_ref.at[b]
        else:
            blocks[b] = found[0]
    lengths = [block.shape[0] - TAIL for block in blocks]
    offsets = [sum(lengths[:b]) for b in range(n_blocks)]

    key_at = lax.broadcasted_iota(jnp.int32, (rows, rows), 0).astype(jnp.float32)
    query_iota = lax.broadcasted_iota(jnp.int32, (rows, rows), 1)
    for block, length, offset in zip(blocks, lengths, offsets):
        tail = block[length : length + TAIL, 0:HEAD_SIZE].astype(jnp.float32)
        for part in range(length // rows):
            high, low = tail[2 * part : 2 * part + 1, :], tail[2 * part + 1 : 2 * part + 2, :]
            key_pos = (high * DIGIT + low)[:, 0:rows] * float(rows) + key_at
            at = slice(offset + part * rows, offset + (part + 1) * rows)
            for i in range(parts):
                query_pos = (query_iota + order_ref[i] * rows).astype(jnp.float32)
                bias_ref[i, at, :] = jnp.where(key_pos > query_pos, HIDDEN, 0.0)
        for k in range(kv_heads):
            at = slice((2 * k + 1) * HEAD_SIZE, (2 * k + 2) * HEAD_SIZE)
            flip_ref[k, :, offset : offset + length] = block[0:length, at].T

    pieces = [
        (k, i, p) for k in range(kv_heads) for i in range(parts) for p in range(heads // pair)
    ]
    tops, totals = {}, {}

    def head_cols(k, p, j):
        head = k * heads + p * pair + j
        return slice(head * HEAD_SIZE, (head + 1) * HEAD_SIZE)

    def score(t):
        k, i, p = pieces[t]
        q = jnp.concatenate(
            [q_ref[i * rows : (i + 1) * rows, head_cols(k, p, j)] for j in range(pair)], axis=0
        )
        top = None
        for block, length, offset in zip(blocks, lengths, offsets):
            key = block[0:length, 2 * k * HEAD_SIZE : (2 * k + 1) * HEAD_SIZE]
            tile = bias_ref[i, offset : offset + length, :]
            scores = lax.dot_general(key, q, NT, preferred_element_type=jnp.float32)
            scores = scores * scale + jnp.concatenate([tile] * pair, axis=1)
            score_refs[t % 2][offset : offset + length, :] = scores
            part = jnp.max(scores, axis=0, keepdims=True)
            top = part if top is None else jnp.maximum(top, part)
        if not first:
            top = jnp.maximum(top, old_top[k * parts + i, :, p * span : (p + 1) * span])
        tops[t] = top

    def weigh(t):
        weights = jnp.exp2(score_refs[t % 2][...] - tops[t])
        totals[t] = jnp.sum(weights, axis=0, keepdims=True)
        weight_refs[t % 2][...] = weights.astype(jnp.bfloat16)

    def spread(t):
        k, i, p = pieces[t]
        at = slice(p * span, (p + 1) * span)
        c = k * parts + i
        acc = jnp.dot(flip_ref[k], weight_refs[t % 2][...], preferred_element_type=jnp.float32)
        total = totals[t]
        if not first:
            factor = jnp.exp2(old_top[c, :, at] - tops[t])
            total = total + old_total[c, :, at] * factor
            acc = acc + old_acc[c, :, at] * factor
        if last:
            done = (acc * (1.0 / total)).astype(jnp.bfloat16).T
            for j in range(pair):
                outs[0][i * rows : (i + 1) * rows, head_cols(k, p, j)] = done[
                    j * rows : (j + 1) * rows, :
                ]
        else:
            outs[0][c, :, at] = tops[t]
            outs[1][c, :, at] = total
            outs[2][c, :, at] = acc

    for t in range(len(pieces) + 2):
        if t < len(pieces):
            score(t)
        if t >= 2:
            spread(t - 2)
        if 1 <= t <= len(pieces):
            weigh(t - 1)
    if last:
        for copy in copies:
            copy.wait()
        multiply_columns(outs[0], buffer, None, products)


def product_shapes(tokens, widths):
    found = []
    for width in widths:
        found.append(jax.ShapeDtypeStruct((tokens, width), jnp.bfloat16))
        found.append(jax.ShapeDtypeStruct((tokens, width), jnp.float32))
    return found


def column_scratch(depth, widths):
    wide = math.gcd(512, *widths)
    tiles = 2 * sum(widths) // wide
    return [pltpu.VMEM((tiles, depth, wide), jnp.bfloat16), pltpu.SemaphoreType.DMA((tiles,))]


def attend(order, queries, blocks, state, kv_heads, then=None):
    tokens, width = queries.shape
    parts = order.shape[0]
    rows = tokens // parts
    heads = width // kv_heads // HEAD_SIZE
    span = math.gcd(heads, 2) * rows
    scale = math.log2(math.e) / math.sqrt(HEAD_SIZE)
    first, last = state is None, then is not None
    seen = sum(block[0].shape[0] - TAIL for block in blocks)
    pairs = tokens * width // HEAD_SIZE * seen
    whole = pl.BlockSpec(memory_space=pltpu.VMEM)
    scalars = pl.BlockSpec(memory_space=pltpu.SMEM)
    combos = kv_heads * parts
    halves = [len(block) for block in blocks]
    arrays = [array for block in blocks for array in block]
    operands = [order, queries, *arrays, *(() if first else state)]
    in_specs = [scalars] + [whole] * (len(operands) - 1)
    scratch = [
        pltpu.VMEM((len(blocks), *arrays[0].shape), arrays[0].dtype),
        pltpu.VMEM((parts, seen, rows), jnp.float32),
        pltpu.VMEM((kv_heads, HEAD_SIZE, seen), jnp.bfloat16),
    ]
    scratch += [pltpu.VMEM((seen, span), jnp.float32)] * 2
    scratch += [pltpu.VMEM((seen, span), jnp.bfloat16)] * 2
    flops = 4 * pairs * HEAD_SIZE
    if last:
        at, weight, widths = then
        operands += [at, weight]
        in_specs += [scalars, pl.BlockSpec(memory_space=pl.ANY)]
        out_shape = [jax.ShapeDtypeStruct(queries.shape, jnp.bfloat16)]
        out_shape += product_shapes(tokens, widths)
        scratch += column_scratch(width, widths)
        flops += 4 * tokens * width * sum(widths)
    else:
        out_shape = [
            jax.ShapeDtypeStruct((combos, 1, heads * rows), jnp.float32),
            jax.ShapeDtypeStruct((combos, 1, heads * rows), jnp.float32),
            jax.ShapeDtypeStruct((combos, HEAD_SIZE, heads * rows), jnp.float32),
        ]
    return pl.pallas_call(
        functools.partial(attend_kernel, halves, first, last, scale, kv_heads, span),
        in_specs=in_specs,
        out_specs=[whole] * len(out_shape),
        out_shape=out_shape,
        scratch_shapes=scratch,
        compiler_params=pltpu.CompilerParams(vmem_limit_bytes=WIDE_LIMIT if last else VMEM_LIMIT),
        cost_estimate=pl.CostEstimate(
            flops=flops, bytes_accessed=4 * pairs, transcendentals=pairs
        ),
    )(*operands)


def project_kernel(at_ref, rows_ref, weight_ref, *refs):
    send_ref, keep_ref, buffer, sem = refs[-4:]
    counts = [out.shape[1] // buffer.shape[2] for out in (send_ref, keep_ref)]
    copies = fetch_columns(at_ref, weight_ref, buffer, sem, counts, DEPTH)
    multiply_columns(rows_ref, buffer, copies, (send_ref, keep_ref))


def project(at, attended, weight, columns, after):
    tokens, depth = attended.shape
    whole = pl.BlockSpec(memory_space=pltpu.VMEM)
    unread = pl.BlockSpec(memory_space=pl.ANY)
    return pl.pallas_call(
        project_kernel,
        in_specs=[pl.BlockSpec(memory_space=pltpu.SMEM), whole, unread] + [unread] * len(after),
        out_specs=[whole] * 2,
        out_shape=product_shapes(tokens, [columns]),
        scratch_shapes=column_scratch(depth, [columns]),
        compiler_params=pltpu.CompilerParams(vmem_limit_bytes=WIDE_LIMIT),
        cost_estimate=pl.CostEstimate(
            flops=4 * tokens * depth * columns,
            bytes_accessed=4 * depth * columns,
            transcendentals=0,
        ),
    )(at, attended, weight, *after)


def add_up_kernel(cuts, n_swapped, mine_ref, *refs):
    out_ref = refs[-1]
    swapped, arrived = refs[:n_swapped], refs[n_swapped:-1]
    each = len(arrived) // (len(cuts) - 1)
    for cut in range(len(cuts) - 1):
        at = slice(cuts[cut], cuts[cut + 1])
        total = mine_ref[:, at]
        for ref in swapped:
            total = total + ref[:, at].astype(jnp.float32)
        for ref in arrived[cut * each : (cut + 1) * each]:
            total = total + ref[...].astype(jnp.float32)
        out_ref[:, at] = total.astype(out_ref.dtype)


def add_up(mine, swapped, arriving, cuts):
    arrived = [x for found in arriving for x in found]
    return pl.pallas_call(
        functools.partial(add_up_kernel, cuts, len(swapped)),
        in_specs=[WHOLE] * (1 + len(swapped) + len(arrived)),
        out_specs=WHOLE,
        out_shape=jax.ShapeDtypeStruct(mine.shape, jnp.bfloat16),
        compiler_params=pltpu.CompilerParams(vmem_limit_bytes=VMEM_LIMIT),
        cost_estimate=pl.CostEstimate(
            flops=4 * mine.size, bytes_accessed=10 * mine.size, transcendentals=0
        ),
    )(mine, *swapped, *arrived)


def shards(n_ctx, n_tp, queries, keys, values, out_weight, block_order):
    heads_dev = queries.shape[1] // HEAD_SIZE
    group_size = QUERY_HEADS // KEY_VALUE_HEADS
    kv_heads = max(1, heads_dev // group_size)
    tp = lax.axis_index("tp")
    start = tp * heads_dev // group_size * HEAD_SIZE
    own_keys = lax.dynamic_slice_in_dim(keys, start, kv_heads * HEAD_SIZE, 1)
    own_values = lax.dynamic_slice_in_dim(values, start, kv_heads * HEAD_SIZE, 1)
    pieces = []
    for head in range(kv_heads):
        at = slice(head * HEAD_SIZE, (head + 1) * HEAD_SIZE)
        pieces += [own_keys[:, at], own_values[:, at]]
    body = jnp.concatenate(pieces, axis=1)
    digits = jnp.stack([block_order // DIGIT, block_order % DIGIT], axis=1).reshape(-1)
    digits = jnp.pad(digits, (0, TAIL - digits.shape[0])).astype(jnp.bfloat16)
    tail = jnp.broadcast_to(digits[:, None], (TAIL, body.shape[1]))
    own = jnp.concatenate([body, tail], axis=0)

    inner = math.gcd(n_ctx, 2)
    outer = n_ctx // inner

    def move(block, target):
        pairs = []
        for o in range(outer):
            for i in range(inner):
                to = target(o, i)
                if to is not None:
                    pairs.append((o * inner + i, to[0] * inner + to[1]))
        return lax.ppermute(block, "ctx", pairs)

    def cross(block, among=None):
        found = []
        for k in range(1, inner):

            def target(o, i):
                return (o, (i + k) % inner) if among is None or o in among else None

            found.append(move(block, target))
        return found

    if outer == 4:
        near = move(own, lambda o, i: (o ^ 1, i))
        opposite = move(own, lambda o, i: (o ^ 2, i))
        mirror = move(own, lambda o, i: (o ^ 3, i))
        stages = [[(own,), (near,)] + [(x,) for x in cross(own)]]
        stages.append([(opposite,)] + [(x,) for x in cross(near)])
        stages.append([(mirror,)] + [(x,) for x in cross(opposite)])
        stages += [[(x,)] for x in cross(mirror)]
    else:
        blocks = [own]
        for k in range(1, outer):
            blocks.append(move(own, lambda o, i: ((o + k) % outer, i)))
        arrived = blocks[1:]
        for k, block in enumerate(blocks):
            arrived += cross(block)
        arrived = [(x,) for x in arrived]
        stages = [[(own,)]]
        stages += [arrived[i : min(i + 3, len(arrived) - 1)] for i in range(0, len(arrived) - 1, 3)]
        stages += [arrived[-1:]] if arrived else []

    share = out_weight.shape[1] // n_tp
    cores = math.gcd(n_tp, 2)
    groups = n_tp // cores
    core, group = tp % cores, tp // cores
    cuts = [0, share // 2, share] if groups == 2 else [0, share]
    widths = [b - a for a, b in zip(cuts, cuts[1:])]
    jobs = [(cut, r) for r in range(1, groups) for cut in range(len(widths))]

    def begins(cut, r):
        to = (group + r) % groups * cores
        firsts = jnp.stack([to + (core + 1) % cores, to + core]) * share
        return (firsts + cuts[cut]).astype(jnp.int32)

    def to_core(x):
        pairs = [(t, t // cores * cores + (t + 1) % cores) for t in range(n_tp)]
        return lax.ppermute(x, "tp", pairs)

    def to_group(x, r):
        pairs = [(t, (t + r * cores) % n_tp) for t in range(n_tp)]
        return lax.ppermute(x, "tp", pairs)

    state = None
    for blocks in stages[:-1]:
        state = attend(block_order, queries, blocks, state, kv_heads)
    cut, r = jobs[0] if jobs else (0, 0)
    attended, send, keep = attend(
        block_order,
        queries,
        stages[-1],
        state,
        kv_heads,
        (begins(cut, r), out_weight, [widths[cut] if jobs else share]),
    )
    arriving = [[] for _ in widths]
    after = ()
    for name, (cut, r) in enumerate(jobs):
        if name > 0:
            send, keep = project(begins(cut, r), attended, out_weight, widths[cut], after)
        if cores > 1:
            keep = keep + to_core(send).astype(jnp.float32)
        total = keep.astype(jnp.bfloat16)
        after = (total,)
        arriving[cut].append(to_group(total, r))
    if jobs:
        send, mine = project(begins(0, 0), attended, out_weight, share, after)
    else:
        mine = keep
    swapped = [to_core(send)] if cores > 1 else []
    return add_up(mine, swapped, arriving, cuts)


def solution(mesh):
    in_specs = (P("ctx", "tp"), P("ctx", None), P("ctx", None), P("tp", None), P("ctx"))
    out_specs = P("ctx", "tp")

    def layer(*args):
        return shards(mesh.shape["ctx"], mesh.shape["tp"], *args)

    return jax.shard_map(
        layer, mesh=mesh, in_specs=in_specs, out_specs=out_specs, check_vma=False
    )
```

```python
import functools
import math

import jax
import jax.numpy as jnp
from jax import lax
from jax.experimental import pallas as pl
from jax.experimental.pallas import tpu as pltpu
from jax.sharding import PartitionSpec as P

QUERY_HEADS = 64
KEY_VALUE_HEADS = 8
HEAD_SIZE = 128
HIDDEN = -1e30
TAIL = 16
DIGIT = 128
WHOLE = pl.BlockSpec(memory_space=pltpu.VMEM)
NT = (((1,), (1,)), ((), ()))
DEPTH = 4
VMEM_LIMIT = 16 << 20
WIDE_LIMIT = 48 << 20


def fetch_columns(at_ref, weight_ref, buffer, sem, counts, started=None):
    wide = buffer.shape[2]
    copies = []
    for run, count in enumerate(counts):
        for tile in range(count):
            column = pl.multiple_of(at_ref[run] + tile * wide, wide)
            n = len(copies)
            copies.append(
                pltpu.make_async_copy(
                    weight_ref.at[:, pl.ds(column, wide)], buffer.at[n], sem.at[n]
                )
            )
    for copy in copies[:started]:
        copy.start()
    return copies


def multiply_columns(rows_ref, buffer, copies, outs):
    wide = buffer.shape[2]
    n = 0
    for out in outs:
        for tile in range(out.shape[1] // wide):
            if copies is not None:
                copies[n].wait()
                if n + DEPTH < len(copies):
                    copies[n + DEPTH].start()
            out[:, tile * wide : (tile + 1) * wide] = jnp.dot(
                rows_ref[...], buffer[n], preferred_element_type=jnp.float32
            ).astype(out.dtype)
            n += 1


def attend_kernel(halves, first, last, scale, kv_heads, span, *refs):
    n_blocks = len(halves)
    order_ref, q_ref = refs[:2]
    blocks, refs = [], refs[2:]
    for count in halves:
        blocks.append(refs[:count])
        refs = refs[count:]
    if not first:
        old_top, old_total, old_acc = refs[:3]
        refs = refs[3:]
    if last:
        at_ref, weight_ref = refs[:2]
        buffer, sem = refs[-2:]
        refs = refs[2:-2]
        products = refs[1:-7]
        counts = [out.shape[1] // buffer.shape[2] for out in products]
        copies = fetch_columns(at_ref, weight_ref, buffer, sem, counts)
    outs = refs[:3]
    merged_ref, bias_ref, flip_ref = refs[-7:-4]
    score_refs, weight_refs = refs[-4:-2], refs[-2:]
    parts = order_ref.shape[0]
    rows = q_ref.shape[0] // parts
    heads = q_ref.shape[1] // kv_heads // HEAD_SIZE
    pair = span // rows
    for b, found in enumerate(blocks):
        if len(found) == 2:
            merged_ref[b] = found[0][...] + found[1][...]
            blocks[b] = merged_ref.at[b]
        else:
            blocks[b] = found[0]
    lengths = [block.shape[0] - TAIL for block in blocks]
    offsets = [sum(lengths[:b]) for b in range(n_blocks)]

    key_at = lax.broadcasted_iota(jnp.int32, (rows, rows), 0).astype(jnp.float32)
    query_iota = lax.broadcasted_iota(jnp.int32, (rows, rows), 1)
    for block, length, offset in zip(blocks, lengths, offsets):
        tail = block[length : length + TAIL, 0:HEAD_SIZE].astype(jnp.float32)
        for part in range(length // rows):
            high, low = tail[2 * part : 2 * part + 1, :], tail[2 * part + 1 : 2 * part + 2, :]
            key_pos = (high * DIGIT + low)[:, 0:rows] * float(rows) + key_at
            at = slice(offset + part * rows, offset + (part + 1) * rows)
            for i in range(parts):
                query_pos = (query_iota + order_ref[i] * rows).astype(jnp.float32)
                bias_ref[i, at, :] = jnp.where(key_pos > query_pos, HIDDEN, 0.0)
        for k in range(kv_heads):
            at = slice((2 * k + 1) * HEAD_SIZE, (2 * k + 2) * HEAD_SIZE)
            flip_ref[k, :, offset : offset + length] = block[0:length, at].T

    pieces = [
        (k, i, p) for k in range(kv_heads) for i in range(parts) for p in range(heads // pair)
    ]
    olds, tops, totals = {}, {}, {}

    def head_cols(k, p, j):
        head = k * heads + p * pair + j
        return slice(head * HEAD_SIZE, (head + 1) * HEAD_SIZE)

    def score(t):
        k, i, p = pieces[t]
        q = jnp.concatenate(
            [q_ref[i * rows : (i + 1) * rows, head_cols(k, p, j)] for j in range(pair)], axis=0
        )
        top = None
        for block, length, offset in zip(blocks, lengths, offsets):
            key = block[0:length, 2 * k * HEAD_SIZE : (2 * k + 1) * HEAD_SIZE]
            tile = bias_ref[i, offset : offset + length, :]
            scores = lax.dot_general(key, q, NT, preferred_element_type=jnp.float32)
            scores = scores * scale + jnp.concatenate([tile] * pair, axis=1)
            score_refs[t % 2][offset : offset + length, :] = scores
            part = jnp.max(scores, axis=0, keepdims=True)
            top = part if top is None else jnp.maximum(top, part)
        if not first:
            olds[t] = old_top[k * parts + i, :, p * span : (p + 1) * span]
            top = jnp.maximum(top, olds[t])
        tops[t] = top

    def weigh(t):
        weights = jnp.exp2(score_refs[t % 2][...] - tops[t])
        totals[t] = jnp.sum(weights, axis=0, keepdims=True)
        weight_refs[t % 2][...] = weights.astype(jnp.bfloat16)

    def spread(t):
        k, i, p = pieces[t]
        at = slice(p * span, (p + 1) * span)
        c = k * parts + i
        acc = jnp.dot(flip_ref[k], weight_refs[t % 2][...], preferred_element_type=jnp.float32)
        total = totals[t]
        if not first:
            factor = jnp.exp2(olds[t] - tops[t])
            total = total + old_total[c, :, at] * factor
            acc = acc + old_acc[c, :, at] * factor
        if last:
            done = (acc * (1.0 / total)).astype(jnp.bfloat16).T
            for j in range(pair):
                outs[0][i * rows : (i + 1) * rows, head_cols(k, p, j)] = done[
                    j * rows : (j + 1) * rows, :
                ]
        else:
            outs[0][c, :, at] = tops[t]
            outs[1][c, :, at] = total
            outs[2][c, :, at] = acc

    for t in range(len(pieces) + 2):
        if t < len(pieces):
            score(t)
        if t >= 2:
            spread(t - 2)
        if 1 <= t <= len(pieces):
            weigh(t - 1)
    if last:
        for copy in copies:
            copy.wait()
        multiply_columns(outs[0], buffer, None, products)


def product_shapes(tokens, widths):
    found = []
    for width in widths:
        found.append(jax.ShapeDtypeStruct((tokens, width), jnp.bfloat16))
        found.append(jax.ShapeDtypeStruct((tokens, width), jnp.float32))
    return found


def column_scratch(depth, widths):
    wide = math.gcd(512, *widths)
    tiles = 2 * sum(widths) // wide
    return [pltpu.VMEM((tiles, depth, wide), jnp.bfloat16), pltpu.SemaphoreType.DMA((tiles,))]


def attend(order, queries, blocks, state, kv_heads, then=None):
    tokens, width = queries.shape
    parts = order.shape[0]
    rows = tokens // parts
    heads = width // kv_heads // HEAD_SIZE
    span = math.gcd(heads, 2) * rows
    scale = math.log2(math.e) / math.sqrt(HEAD_SIZE)
    first, last = state is None, then is not None
    seen = sum(block[0].shape[0] - TAIL for block in blocks)
    pairs = tokens * width // HEAD_SIZE * seen
    whole = pl.BlockSpec(memory_space=pltpu.VMEM)
    scalars = pl.BlockSpec(memory_space=pltpu.SMEM)
    combos = kv_heads * parts
    halves = [len(block) for block in blocks]
    arrays = [array for block in blocks for array in block]
    operands = [order, queries, *arrays, *(() if first else state)]
    in_specs = [scalars] + [whole] * (len(operands) - 1)
    scratch = [
        pltpu.VMEM((len(blocks), *arrays[0].shape), arrays[0].dtype),
        pltpu.VMEM((parts, seen, rows), jnp.float32),
        pltpu.VMEM((kv_heads, HEAD_SIZE, seen), jnp.bfloat16),
    ]
    scratch += [pltpu.VMEM((seen, span), jnp.float32)] * 2
    scratch += [pltpu.VMEM((seen, span), jnp.bfloat16)] * 2
    flops = 4 * pairs * HEAD_SIZE
    if last:
        at, weight, widths = then
        operands += [at, weight]
        in_specs += [scalars, pl.BlockSpec(memory_space=pl.ANY)]
        out_shape = [jax.ShapeDtypeStruct(queries.shape, jnp.bfloat16)]
        out_shape += product_shapes(tokens, widths)
        scratch += column_scratch(width, widths)
        flops += 4 * tokens * width * sum(widths)
    else:
        out_shape = [
            jax.ShapeDtypeStruct((combos, 1, heads * rows), jnp.float32),
            jax.ShapeDtypeStruct((combos, 1, heads * rows), jnp.float32),
            jax.ShapeDtypeStruct((combos, HEAD_SIZE, heads * rows), jnp.float32),
        ]
    return pl.pallas_call(
        functools.partial(attend_kernel, halves, first, last, scale, kv_heads, span),
        in_specs=in_specs,
        out_specs=[whole] * len(out_shape),
        out_shape=out_shape,
        scratch_shapes=scratch,
        input_output_aliases={} if first or last else {2 + len(arrays) + n: n for n in range(3)},
        compiler_params=pltpu.CompilerParams(vmem_limit_bytes=WIDE_LIMIT if last else VMEM_LIMIT),
        cost_estimate=pl.CostEstimate(
            flops=flops, bytes_accessed=4 * pairs, transcendentals=pairs
        ),
    )(*operands)


def project_kernel(at_ref, rows_ref, weight_ref, *refs):
    send_ref, keep_ref, buffer, sem = refs[-4:]
    counts = [out.shape[1] // buffer.shape[2] for out in (send_ref, keep_ref)]
    copies = fetch_columns(at_ref, weight_ref, buffer, sem, counts, DEPTH)
    multiply_columns(rows_ref, buffer, copies, (send_ref, keep_ref))


def project(at, attended, weight, columns, after):
    tokens, depth = attended.shape
    whole = pl.BlockSpec(memory_space=pltpu.VMEM)
    unread = pl.BlockSpec(memory_space=pl.ANY)
    return pl.pallas_call(
        project_kernel,
        in_specs=[pl.BlockSpec(memory_space=pltpu.SMEM), whole, unread] + [unread] * len(after),
        out_specs=[whole] * 2,
        out_shape=product_shapes(tokens, [columns]),
        scratch_shapes=column_scratch(depth, [columns]),
        compiler_params=pltpu.CompilerParams(vmem_limit_bytes=WIDE_LIMIT),
        cost_estimate=pl.CostEstimate(
            flops=4 * tokens * depth * columns,
            bytes_accessed=4 * depth * columns,
            transcendentals=0,
        ),
    )(at, attended, weight, *after)


def add_up_kernel(cuts, n_swapped, mine_ref, *refs):
    out_ref = refs[-1]
    swapped, arrived = refs[:n_swapped], refs[n_swapped:-1]
    each = len(arrived) // (len(cuts) - 1)
    for cut in range(len(cuts) - 1):
        at = slice(cuts[cut], cuts[cut + 1])
        total = mine_ref[:, at]
        for ref in swapped:
            total = total + ref[:, at].astype(jnp.float32)
        for ref in arrived[cut * each : (cut + 1) * each]:
            total = total + ref[...].astype(jnp.float32)
        out_ref[:, at] = total.astype(out_ref.dtype)


def add_up(mine, swapped, arriving, cuts):
    arrived = [x for found in arriving for x in found]
    return pl.pallas_call(
        functools.partial(add_up_kernel, cuts, len(swapped)),
        in_specs=[WHOLE] * (1 + len(swapped) + len(arrived)),
        out_specs=WHOLE,
        out_shape=jax.ShapeDtypeStruct(mine.shape, jnp.bfloat16),
        compiler_params=pltpu.CompilerParams(vmem_limit_bytes=VMEM_LIMIT),
        cost_estimate=pl.CostEstimate(
            flops=4 * mine.size, bytes_accessed=10 * mine.size, transcendentals=0
        ),
    )(mine, *swapped, *arrived)


def shards(n_ctx, n_tp, queries, keys, values, out_weight, block_order):
    heads_dev = queries.shape[1] // HEAD_SIZE
    group_size = QUERY_HEADS // KEY_VALUE_HEADS
    kv_heads = max(1, heads_dev // group_size)
    tp = lax.axis_index("tp")
    start = tp * heads_dev // group_size * HEAD_SIZE
    own_keys = lax.dynamic_slice_in_dim(keys, start, kv_heads * HEAD_SIZE, 1)
    own_values = lax.dynamic_slice_in_dim(values, start, kv_heads * HEAD_SIZE, 1)
    pieces = []
    for head in range(kv_heads):
        at = slice(head * HEAD_SIZE, (head + 1) * HEAD_SIZE)
        pieces += [own_keys[:, at], own_values[:, at]]
    body = jnp.concatenate(pieces, axis=1)
    digits = jnp.stack([block_order // DIGIT, block_order % DIGIT], axis=1).reshape(-1)
    digits = jnp.pad(digits, (0, TAIL - digits.shape[0])).astype(jnp.bfloat16)
    tail = jnp.broadcast_to(digits[:, None], (TAIL, body.shape[1]))
    own = jnp.concatenate([body, tail], axis=0)

    inner = math.gcd(n_ctx, 2)
    outer = n_ctx // inner

    def move(block, target):
        pairs = []
        for o in range(outer):
            for i in range(inner):
                to = target(o, i)
                if to is not None:
                    pairs.append((o * inner + i, to[0] * inner + to[1]))
        return lax.ppermute(block, "ctx", pairs)

    def cross(block, among=None):
        found = []
        for k in range(1, inner):

            def target(o, i):
                return (o, (i + k) % inner) if among is None or o in among else None

            found.append(move(block, target))
        return found

    if outer == 4:
        near = move(own, lambda o, i: (o ^ 1, i))
        opposite = move(own, lambda o, i: (o ^ 2, i))
        mirror = move(own, lambda o, i: (o ^ 3, i))
        stages = [[(own,), (near,)] + [(x,) for x in cross(own)]]
        stages.append([(opposite,)] + [(x,) for x in cross(near)])
        stages.append([(mirror,)] + [(x,) for x in cross(opposite)])
        stages += [[(x,)] for x in cross(mirror)]
    else:
        blocks = [own]
        for k in range(1, outer):
            blocks.append(move(own, lambda o, i: ((o + k) % outer, i)))
        arrived = blocks[1:]
        for k, block in enumerate(blocks):
            arrived += cross(block)
        arrived = [(x,) for x in arrived]
        stages = [[(own,)]]
        stages += [arrived[i : min(i + 3, len(arrived) - 1)] for i in range(0, len(arrived) - 1, 3)]
        stages += [arrived[-1:]] if arrived else []

    share = out_weight.shape[1] // n_tp
    cores = math.gcd(n_tp, 2)
    groups = n_tp // cores
    core, group = tp % cores, tp // cores
    cuts = [0, share // 2, share] if groups == 2 else [0, share]
    widths = [b - a for a, b in zip(cuts, cuts[1:])]
    jobs = [(cut, r) for r in range(1, groups) for cut in range(len(widths))]

    def begins(cut, r):
        to = (group + r) % groups * cores
        firsts = jnp.stack([to + (core + 1) % cores, to + core]) * share
        return (firsts + cuts[cut]).astype(jnp.int32)

    def to_core(x):
        pairs = [(t, t // cores * cores + (t + 1) % cores) for t in range(n_tp)]
        return lax.ppermute(x, "tp", pairs)

    def to_group(x, r):
        pairs = [(t, (t + r * cores) % n_tp) for t in range(n_tp)]
        return lax.ppermute(x, "tp", pairs)

    state = None
    for blocks in stages[:-1]:
        state = attend(block_order, queries, blocks, state, kv_heads)
    cut, r = jobs[0] if jobs else (0, 0)
    attended, send, keep = attend(
        block_order,
        queries,
        stages[-1],
        state,
        kv_heads,
        (begins(cut, r), out_weight, [widths[cut] if jobs else share]),
    )
    arriving = [[] for _ in widths]
    after = ()
    for name, (cut, r) in enumerate(jobs):
        if name > 0:
            send, keep = project(begins(cut, r), attended, out_weight, widths[cut], after)
        if cores > 1:
            keep = keep + to_core(send).astype(jnp.float32)
        total = keep.astype(jnp.bfloat16)
        after = (total,)
        arriving[cut].append(to_group(total, r))
    if jobs:
        send, mine = project(begins(0, 0), attended, out_weight, share, after)
    else:
        mine = keep
    swapped = [to_core(send)] if cores > 1 else []
    return add_up(mine, swapped, arriving, cuts)


def solution(mesh):
    in_specs = (P("ctx", "tp"), P("ctx", None), P("ctx", None), P("tp", None), P("ctx"))
    out_specs = P("ctx", "tp")

    def layer(*args):
        return shards(mesh.shape["ctx"], mesh.shape["tp"], *args)

    return jax.shard_map(
        layer, mesh=mesh, in_specs=in_specs, out_specs=out_specs, check_vma=False
    )
```

```python
import functools
import math

import jax
import jax.numpy as jnp
from jax import lax
from jax.experimental import pallas as pl
from jax.experimental.pallas import tpu as pltpu
from jax.sharding import PartitionSpec as P

QUERY_HEADS = 64
KEY_VALUE_HEADS = 8
HEAD_SIZE = 128
HIDDEN = -1e30
TAIL = 16
DIGIT = 128
WHOLE = pl.BlockSpec(memory_space=pltpu.VMEM)
NT = (((1,), (1,)), ((), ()))
DEPTH = 4
VMEM_LIMIT = 16 << 20
WIDE_LIMIT = 48 << 20


def fetch_columns(at_ref, weight_ref, buffer, sem, counts, started=None):
    wide = buffer.shape[2]
    copies = []
    for run, count in enumerate(counts):
        for tile in range(count):
            column = pl.multiple_of(at_ref[run] + tile * wide, wide)
            n = len(copies)
            copies.append(
                pltpu.make_async_copy(
                    weight_ref.at[:, pl.ds(column, wide)], buffer.at[n], sem.at[n]
                )
            )
    for copy in copies[:started]:
        copy.start()
    return copies


def multiply_columns(rows_ref, buffer, copies, outs):
    wide = buffer.shape[2]
    n = 0
    for out in outs:
        for tile in range(out.shape[1] // wide):
            if copies is not None:
                copies[n].wait()
                if n + DEPTH < len(copies):
                    copies[n + DEPTH].start()
            out[:, tile * wide : (tile + 1) * wide] = jnp.dot(
                rows_ref[...], buffer[n], preferred_element_type=jnp.float32
            ).astype(out.dtype)
            n += 1


def attend_kernel(halves, first, last, scale, kv_heads, span, *refs):
    n_blocks = len(halves)
    order_ref, q_ref = refs[:2]
    blocks, refs = [], refs[2:]
    for count in halves:
        blocks.append(refs[:count])
        refs = refs[count:]
    if not first:
        old_top, old_total, old_acc = refs[:3]
        refs = refs[3:]
    if last:
        at_ref, weight_ref = refs[:2]
        buffer, sem = refs[-2:]
        refs = refs[2:-2]
        products = refs[1:-7]
        counts = [out.shape[1] // buffer.shape[2] for out in products]
        copies = fetch_columns(at_ref, weight_ref, buffer, sem, counts)
    outs = refs[:3]
    merged_ref, bias_ref, flip_ref = refs[-7:-4]
    score_refs, weight_refs = refs[-4:-2], refs[-2:]
    parts = order_ref.shape[0]
    rows = q_ref.shape[0] // parts
    heads = q_ref.shape[1] // kv_heads // HEAD_SIZE
    pair = span // rows
    for b, found in enumerate(blocks):
        if len(found) == 2:
            merged_ref[b] = found[0][...] + found[1][...]
            blocks[b] = merged_ref.at[b]
        else:
            blocks[b] = found[0]
    lengths = [block.shape[0] - TAIL for block in blocks]
    offsets = [sum(lengths[:b]) for b in range(n_blocks)]

    key_at = lax.broadcasted_iota(jnp.int32, (rows, rows), 0).astype(jnp.float32)
    query_iota = lax.broadcasted_iota(jnp.int32, (rows, rows), 1)
    for block, length, offset in zip(blocks, lengths, offsets):
        tail = block[length : length + TAIL, 0:HEAD_SIZE].astype(jnp.float32)
        for part in range(length // rows):
            high, low = tail[2 * part : 2 * part + 1, :], tail[2 * part + 1 : 2 * part + 2, :]
            key_pos = (high * DIGIT + low)[:, 0:rows] * float(rows) + key_at
            at = slice(offset + part * rows, offset + (part + 1) * rows)
            for i in range(parts):
                query_pos = (query_iota + order_ref[i] * rows).astype(jnp.float32)
                bias_ref[i, at, :] = jnp.where(key_pos > query_pos, HIDDEN, 0.0)
        for k in range(kv_heads):
            at = slice((2 * k + 1) * HEAD_SIZE, (2 * k + 2) * HEAD_SIZE)
            flip_ref[k, :, offset : offset + length] = block[0:length, at].T

    pieces = [
        (k, i, p) for k in range(kv_heads) for i in range(parts) for p in range(heads // pair)
    ]
    olds, tops, totals = {}, {}, {}

    def head_cols(k, p, j):
        head = k * heads + p * pair + j
        return slice(head * HEAD_SIZE, (head + 1) * HEAD_SIZE)

    def score(t):
        k, i, p = pieces[t]
        q = jnp.concatenate(
            [q_ref[i * rows : (i + 1) * rows, head_cols(k, p, j)] for j in range(pair)], axis=0
        )
        top = None
        for block, length, offset in zip(blocks, lengths, offsets):
            key = block[0:length, 2 * k * HEAD_SIZE : (2 * k + 1) * HEAD_SIZE]
            tile = bias_ref[i, offset : offset + length, :]
            scores = lax.dot_general(key, q, NT, preferred_element_type=jnp.float32)
            scores = scores * scale + jnp.concatenate([tile] * pair, axis=1)
            score_refs[t % 2][offset : offset + length, :] = scores
            part = jnp.max(scores, axis=0, keepdims=True)
            top = part if top is None else jnp.maximum(top, part)
        if not first:
            olds[t] = old_top[k * parts + i, :, p * span : (p + 1) * span]
            top = jnp.maximum(top, olds[t])
        tops[t] = top

    def weigh(t):
        weights = jnp.exp2(score_refs[t % 2][...] - tops[t])
        totals[t] = jnp.sum(weights, axis=0, keepdims=True)
        weight_refs[t % 2][...] = weights.astype(jnp.bfloat16)

    def spread(t):
        k, i, p = pieces[t]
        at = slice(p * span, (p + 1) * span)
        c = k * parts + i
        acc = jnp.dot(flip_ref[k], weight_refs[t % 2][...], preferred_element_type=jnp.float32)
        total = totals[t]
        if not first:
            factor = jnp.exp2(olds[t] - tops[t])
            total = total + old_total[c, :, at] * factor
            acc = acc + old_acc[c, :, at] * factor
        if last:
            done = (acc * (1.0 / total)).astype(jnp.bfloat16).T
            for j in range(pair):
                outs[0][i * rows : (i + 1) * rows, head_cols(k, p, j)] = done[
                    j * rows : (j + 1) * rows, :
                ]
        else:
            outs[0][c, :, at] = tops[t]
            outs[1][c, :, at] = total
            outs[2][c, :, at] = acc

    for t in range(len(pieces) + 2):
        if t < len(pieces):
            score(t)
        if t >= 2:
            spread(t - 2)
        if 1 <= t <= len(pieces):
            weigh(t - 1)
    if last:
        for copy in copies:
            copy.wait()
        multiply_columns(outs[0], buffer, None, products)


def product_shapes(tokens, widths):
    found = []
    for width in widths:
        found.append(jax.ShapeDtypeStruct((tokens, width), jnp.bfloat16))
        found.append(jax.ShapeDtypeStruct((tokens, width), jnp.float32))
    return found


def column_scratch(depth, widths):
    wide = math.gcd(512, *widths)
    tiles = 2 * sum(widths) // wide
    return [pltpu.VMEM((tiles, depth, wide), jnp.bfloat16), pltpu.SemaphoreType.DMA((tiles,))]


def attend(order, queries, blocks, state, kv_heads, then=None):
    tokens, width = queries.shape
    parts = order.shape[0]
    rows = tokens // parts
    heads = width // kv_heads // HEAD_SIZE
    span = math.gcd(heads, 2) * rows
    scale = math.log2(math.e) / math.sqrt(HEAD_SIZE)
    first, last = state is None, then is not None
    seen = sum(block[0].shape[0] - TAIL for block in blocks)
    pairs = tokens * width // HEAD_SIZE * seen
    whole = pl.BlockSpec(memory_space=pltpu.VMEM)
    scalars = pl.BlockSpec(memory_space=pltpu.SMEM)
    combos = kv_heads * parts
    halves = [len(block) for block in blocks]
    arrays = [array for block in blocks for array in block]
    operands = [order, queries, *arrays, *(() if first else state)]
    in_specs = [scalars] + [whole] * (len(operands) - 1)
    scratch = [
        pltpu.VMEM((len(blocks), *arrays[0].shape), arrays[0].dtype),
        pltpu.VMEM((parts, seen, rows), jnp.float32),
        pltpu.VMEM((kv_heads, HEAD_SIZE, seen), jnp.bfloat16),
    ]
    scratch += [pltpu.VMEM((seen, span), jnp.float32)] * 2
    scratch += [pltpu.VMEM((seen, span), jnp.bfloat16)] * 2
    flops = 4 * pairs * HEAD_SIZE
    if last:
        at, weight, widths = then
        operands += [at, weight]
        in_specs += [scalars, pl.BlockSpec(memory_space=pl.ANY)]
        out_shape = [jax.ShapeDtypeStruct(queries.shape, jnp.bfloat16)]
        out_shape += product_shapes(tokens, widths)
        scratch += column_scratch(width, widths)
        flops += 4 * tokens * width * sum(widths)
    else:
        out_shape = [
            jax.ShapeDtypeStruct((combos, 1, heads * rows), jnp.float32),
            jax.ShapeDtypeStruct((combos, 1, heads * rows), jnp.float32),
            jax.ShapeDtypeStruct((combos, HEAD_SIZE, heads * rows), jnp.float32),
        ]
    return pl.pallas_call(
        functools.partial(attend_kernel, halves, first, last, scale, kv_heads, span),
        in_specs=in_specs,
        out_specs=[whole] * len(out_shape),
        out_shape=out_shape,
        scratch_shapes=scratch,
        input_output_aliases={} if first or last else {2 + len(arrays) + n: n for n in range(3)},
        compiler_params=pltpu.CompilerParams(vmem_limit_bytes=WIDE_LIMIT if last else VMEM_LIMIT),
        cost_estimate=pl.CostEstimate(
            flops=flops, bytes_accessed=4 * pairs, transcendentals=pairs
        ),
    )(*operands)


def project_kernel(at_ref, rows_ref, weight_ref, *refs):
    send_ref, keep_ref, buffer, sem = refs[-4:]
    counts = [out.shape[1] // buffer.shape[2] for out in (send_ref, keep_ref)]
    copies = fetch_columns(at_ref, weight_ref, buffer, sem, counts, DEPTH)
    multiply_columns(rows_ref, buffer, copies, (send_ref, keep_ref))


def project(at, attended, weight, columns, after):
    tokens, depth = attended.shape
    whole = pl.BlockSpec(memory_space=pltpu.VMEM)
    unread = pl.BlockSpec(memory_space=pl.ANY)
    return pl.pallas_call(
        project_kernel,
        in_specs=[pl.BlockSpec(memory_space=pltpu.SMEM), whole, unread] + [unread] * len(after),
        out_specs=[whole] * 2,
        out_shape=product_shapes(tokens, [columns]),
        scratch_shapes=column_scratch(depth, [columns]),
        compiler_params=pltpu.CompilerParams(vmem_limit_bytes=WIDE_LIMIT),
        cost_estimate=pl.CostEstimate(
            flops=4 * tokens * depth * columns,
            bytes_accessed=4 * depth * columns,
            transcendentals=0,
        ),
    )(at, attended, weight, *after)


def add_up_kernel(cuts, n_swapped, mine_ref, *refs):
    out_ref = refs[-1]
    swapped, arrived = refs[:n_swapped], refs[n_swapped:-1]
    each = len(arrived) // (len(cuts) - 1)
    for cut in range(len(cuts) - 1):
        at = slice(cuts[cut], cuts[cut + 1])
        total = mine_ref[:, at]
        for ref in swapped:
            total = total + ref[:, at].astype(jnp.float32)
        for ref in arrived[cut * each : (cut + 1) * each]:
            total = total + ref[...].astype(jnp.float32)
        out_ref[:, at] = total.astype(out_ref.dtype)


def add_up(mine, swapped, arriving, cuts):
    arrived = [x for found in arriving for x in found]
    return pl.pallas_call(
        functools.partial(add_up_kernel, cuts, len(swapped)),
        in_specs=[WHOLE] * (1 + len(swapped) + len(arrived)),
        out_specs=WHOLE,
        out_shape=jax.ShapeDtypeStruct(mine.shape, jnp.bfloat16),
        compiler_params=pltpu.CompilerParams(vmem_limit_bytes=VMEM_LIMIT),
        cost_estimate=pl.CostEstimate(
            flops=4 * mine.size, bytes_accessed=10 * mine.size, transcendentals=0
        ),
    )(mine, *swapped, *arrived)


def shards(n_ctx, n_tp, queries, keys, values, out_weight, block_order):
    heads_dev = queries.shape[1] // HEAD_SIZE
    group_size = QUERY_HEADS // KEY_VALUE_HEADS
    kv_heads = max(1, heads_dev // group_size)
    tp = lax.axis_index("tp")
    start = tp * heads_dev // group_size * HEAD_SIZE
    own_keys = lax.dynamic_slice_in_dim(keys, start, kv_heads * HEAD_SIZE, 1)
    own_values = lax.dynamic_slice_in_dim(values, start, kv_heads * HEAD_SIZE, 1)
    pieces = []
    for head in range(kv_heads):
        at = slice(head * HEAD_SIZE, (head + 1) * HEAD_SIZE)
        pieces += [own_keys[:, at], own_values[:, at]]
    body = jnp.concatenate(pieces, axis=1)
    digits = jnp.stack([block_order // DIGIT, block_order % DIGIT], axis=1).reshape(-1)
    digits = jnp.pad(digits, (0, TAIL - digits.shape[0])).astype(jnp.bfloat16)
    tail = jnp.broadcast_to(digits[:, None], (TAIL, body.shape[1]))
    own = jnp.concatenate([body, tail], axis=0)

    inner = math.gcd(n_ctx, 2)
    outer = n_ctx // inner

    def move(block, target):
        pairs = []
        for o in range(outer):
            for i in range(inner):
                to = target(o, i)
                if to is not None:
                    pairs.append((o * inner + i, to[0] * inner + to[1]))
        return lax.ppermute(block, "ctx", pairs)

    def cross(block, among=None):
        found = []
        for k in range(1, inner):

            def target(o, i):
                return (o, (i + k) % inner) if among is None or o in among else None

            found.append(move(block, target))
        return found

    if outer == 4:
        near = move(own, lambda o, i: (o ^ 1, i))
        opposite = move(own, lambda o, i: (o ^ 2, i))
        mirror = move(own, lambda o, i: (o ^ 3, i))
        own_crossed = [(x,) for x in cross(own)]
        near_crossed = [(x,) for x in cross(near)]
        opposite_crossed = [(x,) for x in cross(opposite)]
        stages = [[(own,)], [(near,)] + own_crossed + [(opposite,)]]
        stages.append(near_crossed + [(mirror,)] + opposite_crossed)
        stages += [[(x,)] for x in cross(mirror)]
    else:
        blocks = [own]
        for k in range(1, outer):
            blocks.append(move(own, lambda o, i: ((o + k) % outer, i)))
        arrived = blocks[1:]
        for k, block in enumerate(blocks):
            arrived += cross(block)
        arrived = [(x,) for x in arrived]
        stages = [[(own,)]]
        stages += [arrived[i : min(i + 3, len(arrived) - 1)] for i in range(0, len(arrived) - 1, 3)]
        stages += [arrived[-1:]] if arrived else []

    share = out_weight.shape[1] // n_tp
    cores = math.gcd(n_tp, 2)
    groups = n_tp // cores
    core, group = tp % cores, tp // cores
    cuts = [0, share // 2, share] if groups == 2 else [0, share]
    widths = [b - a for a, b in zip(cuts, cuts[1:])]
    jobs = [(cut, r) for r in range(1, groups) for cut in range(len(widths))]

    def begins(cut, r):
        to = (group + r) % groups * cores
        firsts = jnp.stack([to + (core + 1) % cores, to + core]) * share
        return (firsts + cuts[cut]).astype(jnp.int32)

    def to_core(x):
        pairs = [(t, t // cores * cores + (t + 1) % cores) for t in range(n_tp)]
        return lax.ppermute(x, "tp", pairs)

    def to_group(x, r):
        pairs = [(t, (t + r * cores) % n_tp) for t in range(n_tp)]
        return lax.ppermute(x, "tp", pairs)

    state = None
    for blocks in stages[:-1]:
        state = attend(block_order, queries, blocks, state, kv_heads)
    cut, r = jobs[0] if jobs else (0, 0)
    attended, send, keep = attend(
        block_order,
        queries,
        stages[-1],
        state,
        kv_heads,
        (begins(cut, r), out_weight, [widths[cut] if jobs else share]),
    )
    arriving = [[] for _ in widths]
    after = ()
    for name, (cut, r) in enumerate(jobs):
        if name > 0:
            send, keep = project(begins(cut, r), attended, out_weight, widths[cut], after)
        if cores > 1:
            keep = keep + to_core(send).astype(jnp.float32)
        total = keep.astype(jnp.bfloat16)
        after = (total,)
        arriving[cut].append(to_group(total, r))
    if jobs:
        send, mine = project(begins(0, 0), attended, out_weight, share, after)
    else:
        mine = keep
    swapped = [to_core(send)] if cores > 1 else []
    return add_up(mine, swapped, arriving, cuts)


def solution(mesh):
    in_specs = (P("ctx", "tp"), P("ctx", None), P("ctx", None), P("tp", None), P("ctx"))
    out_specs = P("ctx", "tp")

    def layer(*args):
        return shards(mesh.shape["ctx"], mesh.shape["tp"], *args)

    return jax.shard_map(
        layer, mesh=mesh, in_specs=in_specs, out_specs=out_specs, check_vma=False
    )
```

```python
import functools
import math

import jax
import jax.numpy as jnp
from jax import lax
from jax.experimental import pallas as pl
from jax.experimental.pallas import tpu as pltpu
from jax.sharding import PartitionSpec as P

QUERY_HEADS = 64
KEY_VALUE_HEADS = 8
HEAD_SIZE = 128
HIDDEN = -1e30
TAIL = 16
DIGIT = 128
WHOLE = pl.BlockSpec(memory_space=pltpu.VMEM)
NT = (((1,), (1,)), ((), ()))
DEPTH = 4
VMEM_LIMIT = 16 << 20
WIDE_LIMIT = 48 << 20


def fetch_columns(at_ref, weight_ref, buffer, sem, counts, started=None):
    wide = buffer.shape[2]
    copies = []
    for run, count in enumerate(counts):
        for tile in range(count):
            column = pl.multiple_of(at_ref[run] + tile * wide, wide)
            n = len(copies)
            copies.append(
                pltpu.make_async_copy(
                    weight_ref.at[:, pl.ds(column, wide)], buffer.at[n], sem.at[n]
                )
            )
    for copy in copies[:started]:
        copy.start()
    return copies


def multiply_columns(rows_ref, buffer, copies, outs):
    wide = buffer.shape[2]
    n = 0
    for out in outs:
        for tile in range(out.shape[1] // wide):
            if copies is not None:
                copies[n].wait()
                if n + DEPTH < len(copies):
                    copies[n + DEPTH].start()
            out[:, tile * wide : (tile + 1) * wide] = jnp.dot(
                rows_ref[...], buffer[n], preferred_element_type=jnp.float32
            ).astype(out.dtype)
            n += 1


def attend_kernel(halves, first, last, scale, kv_heads, span, *refs):
    n_blocks = len(halves)
    order_ref, q_ref = refs[:2]
    blocks, refs = [], refs[2:]
    for count in halves:
        blocks.append(refs[:count])
        refs = refs[count:]
    if not first:
        old_top, old_total, old_acc = refs[:3]
        refs = refs[3:]
    if last:
        at_ref, weight_ref = refs[:2]
        buffer, sem = refs[-2:]
        refs = refs[2:-2]
        products = refs[1:-7]
        counts = [out.shape[1] // buffer.shape[2] for out in products]
        copies = fetch_columns(at_ref, weight_ref, buffer, sem, counts)
    outs = refs[:3]
    merged_ref, bias_ref, flip_ref = refs[-7:-4]
    score_refs, weight_refs = refs[-4:-2], refs[-2:]
    parts = order_ref.shape[0]
    rows = q_ref.shape[0] // parts
    heads = q_ref.shape[1] // kv_heads // HEAD_SIZE
    pair = span // rows
    for b, found in enumerate(blocks):
        if len(found) == 2:
            merged_ref[b] = found[0][...] + found[1][...]
            blocks[b] = merged_ref.at[b]
        else:
            blocks[b] = found[0]
    lengths = [block.shape[0] - TAIL for block in blocks]
    offsets = [sum(lengths[:b]) for b in range(n_blocks)]

    key_at = lax.broadcasted_iota(jnp.int32, (rows, rows), 0).astype(jnp.float32)
    query_iota = lax.broadcasted_iota(jnp.int32, (rows, rows), 1)
    for block, length, offset in zip(blocks, lengths, offsets):
        tail = block[length : length + TAIL, 0:HEAD_SIZE].astype(jnp.float32)
        for part in range(length // rows):
            high, low = tail[2 * part : 2 * part + 1, :], tail[2 * part + 1 : 2 * part + 2, :]
            key_pos = (high * DIGIT + low)[:, 0:rows] * float(rows) + key_at
            at = slice(offset + part * rows, offset + (part + 1) * rows)
            for i in range(parts):
                query_pos = (query_iota + order_ref[i] * rows).astype(jnp.float32)
                bias_ref[i, at, :] = jnp.where(key_pos > query_pos, HIDDEN, 0.0)
        for k in range(kv_heads):
            at = slice((2 * k + 1) * HEAD_SIZE, (2 * k + 2) * HEAD_SIZE)
            flip_ref[k, :, offset : offset + length] = block[0:length, at].T

    pieces = [
        (k, i, p) for k in range(kv_heads) for i in range(parts) for p in range(heads // pair)
    ]
    olds, tops, totals = {}, {}, {}

    def head_cols(k, p, j):
        head = k * heads + p * pair + j
        return slice(head * HEAD_SIZE, (head + 1) * HEAD_SIZE)

    def score(t):
        k, i, p = pieces[t]
        q = jnp.concatenate(
            [q_ref[i * rows : (i + 1) * rows, head_cols(k, p, j)] for j in range(pair)], axis=0
        )
        top = None
        for block, length, offset in zip(blocks, lengths, offsets):
            key = block[0:length, 2 * k * HEAD_SIZE : (2 * k + 1) * HEAD_SIZE]
            tile = bias_ref[i, offset : offset + length, :]
            scores = lax.dot_general(key, q, NT, preferred_element_type=jnp.float32)
            scores = scores * scale + jnp.concatenate([tile] * pair, axis=1)
            score_refs[t % 2][offset : offset + length, :] = scores
            part = jnp.max(scores, axis=0, keepdims=True)
            top = part if top is None else jnp.maximum(top, part)
        if not first:
            olds[t] = old_top[k * parts + i, :, p * span : (p + 1) * span]
            top = jnp.maximum(top, olds[t])
        tops[t] = top

    def weigh(t):
        weights = jnp.exp2(score_refs[t % 2][...] - tops[t])
        totals[t] = jnp.sum(weights, axis=0, keepdims=True)
        weight_refs[t % 2][...] = weights.astype(jnp.bfloat16)

    def spread(t):
        k, i, p = pieces[t]
        at = slice(p * span, (p + 1) * span)
        c = k * parts + i
        acc = jnp.dot(flip_ref[k], weight_refs[t % 2][...], preferred_element_type=jnp.float32)
        total = totals[t]
        if not first:
            factor = jnp.exp2(olds[t] - tops[t])
            total = total + old_total[c, :, at] * factor
            acc = acc + old_acc[c, :, at] * factor
        if last:
            done = (acc * (1.0 / total)).astype(jnp.bfloat16).T
            for j in range(pair):
                outs[0][i * rows : (i + 1) * rows, head_cols(k, p, j)] = done[
                    j * rows : (j + 1) * rows, :
                ]
        else:
            outs[0][c, :, at] = tops[t]
            outs[1][c, :, at] = total
            outs[2][c, :, at] = acc

    for t in range(len(pieces) + 2):
        if t < len(pieces):
            score(t)
        if t >= 2:
            spread(t - 2)
        if 1 <= t <= len(pieces):
            weigh(t - 1)
    if last:
        for copy in copies:
            copy.wait()
        multiply_columns(outs[0], buffer, None, products)


def product_shapes(tokens, widths):
    found = []
    for width in widths:
        found.append(jax.ShapeDtypeStruct((tokens, width), jnp.bfloat16))
        found.append(jax.ShapeDtypeStruct((tokens, width), jnp.float32))
    return found


def column_scratch(depth, widths):
    wide = math.gcd(512, *widths)
    tiles = 2 * sum(widths) // wide
    return [pltpu.VMEM((tiles, depth, wide), jnp.bfloat16), pltpu.SemaphoreType.DMA((tiles,))]


def attend(order, queries, blocks, state, kv_heads, then=None):
    tokens, width = queries.shape
    parts = order.shape[0]
    rows = tokens // parts
    heads = width // kv_heads // HEAD_SIZE
    span = math.gcd(heads, 2) * rows
    scale = math.log2(math.e) / math.sqrt(HEAD_SIZE)
    first, last = state is None, then is not None
    seen = sum(block[0].shape[0] - TAIL for block in blocks)
    pairs = tokens * width // HEAD_SIZE * seen
    whole = pl.BlockSpec(memory_space=pltpu.VMEM)
    scalars = pl.BlockSpec(memory_space=pltpu.SMEM)
    combos = kv_heads * parts
    halves = [len(block) for block in blocks]
    arrays = [array for block in blocks for array in block]
    operands = [order, queries, *arrays, *(() if first else state)]
    in_specs = [scalars] + [whole] * (len(operands) - 1)
    scratch = [
        pltpu.VMEM((len(blocks), *arrays[0].shape), arrays[0].dtype),
        pltpu.VMEM((parts, seen, rows), jnp.float32),
        pltpu.VMEM((kv_heads, HEAD_SIZE, seen), jnp.bfloat16),
    ]
    scratch += [pltpu.VMEM((seen, span), jnp.float32)] * 2
    scratch += [pltpu.VMEM((seen, span), jnp.bfloat16)] * 2
    flops = 4 * pairs * HEAD_SIZE
    if last:
        at, weight, widths = then
        operands += [at, weight]
        in_specs += [scalars, pl.BlockSpec(memory_space=pl.ANY)]
        out_shape = [jax.ShapeDtypeStruct(queries.shape, jnp.bfloat16)]
        out_shape += product_shapes(tokens, widths)
        scratch += column_scratch(width, widths)
        flops += 4 * tokens * width * sum(widths)
    else:
        out_shape = [
            jax.ShapeDtypeStruct((combos, 1, heads * rows), jnp.float32),
            jax.ShapeDtypeStruct((combos, 1, heads * rows), jnp.float32),
            jax.ShapeDtypeStruct((combos, HEAD_SIZE, heads * rows), jnp.float32),
        ]
    return pl.pallas_call(
        functools.partial(attend_kernel, halves, first, last, scale, kv_heads, span),
        in_specs=in_specs,
        out_specs=[whole] * len(out_shape),
        out_shape=out_shape,
        scratch_shapes=scratch,
        compiler_params=pltpu.CompilerParams(vmem_limit_bytes=WIDE_LIMIT if last else VMEM_LIMIT),
        cost_estimate=pl.CostEstimate(
            flops=flops, bytes_accessed=4 * pairs, transcendentals=pairs
        ),
    )(*operands)


def project_kernel(at_ref, rows_ref, weight_ref, *refs):
    send_ref, keep_ref, buffer, sem = refs[-4:]
    counts = [out.shape[1] // buffer.shape[2] for out in (send_ref, keep_ref)]
    copies = fetch_columns(at_ref, weight_ref, buffer, sem, counts, DEPTH)
    multiply_columns(rows_ref, buffer, copies, (send_ref, keep_ref))


def project(at, attended, weight, columns, after):
    tokens, depth = attended.shape
    whole = pl.BlockSpec(memory_space=pltpu.VMEM)
    unread = pl.BlockSpec(memory_space=pl.ANY)
    return pl.pallas_call(
        project_kernel,
        in_specs=[pl.BlockSpec(memory_space=pltpu.SMEM), whole, unread] + [unread] * len(after),
        out_specs=[whole] * 2,
        out_shape=product_shapes(tokens, [columns]),
        scratch_shapes=column_scratch(depth, [columns]),
        compiler_params=pltpu.CompilerParams(vmem_limit_bytes=WIDE_LIMIT),
        cost_estimate=pl.CostEstimate(
            flops=4 * tokens * depth * columns,
            bytes_accessed=4 * depth * columns,
            transcendentals=0,
        ),
    )(at, attended, weight, *after)


def add_up_kernel(cuts, n_swapped, mine_ref, *refs):
    out_ref = refs[-1]
    swapped, arrived = refs[:n_swapped], refs[n_swapped:-1]
    each = len(arrived) // (len(cuts) - 1)
    for cut in range(len(cuts) - 1):
        at = slice(cuts[cut], cuts[cut + 1])
        total = mine_ref[:, at]
        for ref in swapped:
            total = total + ref[:, at].astype(jnp.float32)
        for ref in arrived[cut * each : (cut + 1) * each]:
            total = total + ref[...].astype(jnp.float32)
        out_ref[:, at] = total.astype(out_ref.dtype)


def add_up(mine, swapped, arriving, cuts):
    arrived = [x for found in arriving for x in found]
    return pl.pallas_call(
        functools.partial(add_up_kernel, cuts, len(swapped)),
        in_specs=[WHOLE] * (1 + len(swapped) + len(arrived)),
        out_specs=WHOLE,
        out_shape=jax.ShapeDtypeStruct(mine.shape, jnp.bfloat16),
        compiler_params=pltpu.CompilerParams(vmem_limit_bytes=VMEM_LIMIT),
        cost_estimate=pl.CostEstimate(
            flops=4 * mine.size, bytes_accessed=10 * mine.size, transcendentals=0
        ),
    )(mine, *swapped, *arrived)


def shards(n_ctx, n_tp, queries, keys, values, out_weight, block_order):
    heads_dev = queries.shape[1] // HEAD_SIZE
    group_size = QUERY_HEADS // KEY_VALUE_HEADS
    kv_heads = max(1, heads_dev // group_size)
    tp = lax.axis_index("tp")
    start = tp * heads_dev // group_size * HEAD_SIZE
    own_keys = lax.dynamic_slice_in_dim(keys, start, kv_heads * HEAD_SIZE, 1)
    own_values = lax.dynamic_slice_in_dim(values, start, kv_heads * HEAD_SIZE, 1)
    pieces = []
    for head in range(kv_heads):
        at = slice(head * HEAD_SIZE, (head + 1) * HEAD_SIZE)
        pieces += [own_keys[:, at], own_values[:, at]]
    body = jnp.concatenate(pieces, axis=1)
    digits = jnp.stack([block_order // DIGIT, block_order % DIGIT], axis=1).reshape(-1)
    digits = jnp.pad(digits, (0, TAIL - digits.shape[0])).astype(jnp.bfloat16)
    tail = jnp.broadcast_to(digits[:, None], (TAIL, body.shape[1]))
    own = jnp.concatenate([body, tail], axis=0)

    inner = math.gcd(n_ctx, 2)
    outer = n_ctx // inner

    def move(block, target):
        pairs = []
        for o in range(outer):
            for i in range(inner):
                to = target(o, i)
                if to is not None:
                    pairs.append((o * inner + i, to[0] * inner + to[1]))
        return lax.ppermute(block, "ctx", pairs)

    def cross(block, among=None):
        found = []
        for k in range(1, inner):

            def target(o, i):
                return (o, (i + k) % inner) if among is None or o in among else None

            found.append(move(block, target))
        return found

    if outer == 4:
        near = move(own, lambda o, i: (o ^ 1, i))
        opposite = move(own, lambda o, i: (o ^ 2, i))
        mirror = move(own, lambda o, i: (o ^ 3, i))
        own_crossed = [(x,) for x in cross(own)]
        near_crossed = [(x,) for x in cross(near)]
        opposite_crossed = [(x,) for x in cross(opposite)]
        stages = [[(own,)], [(near,)] + own_crossed + [(opposite,)]]
        stages.append(near_crossed + [(mirror,)])
        stages.append(opposite_crossed + [(x,) for x in cross(mirror)])
    else:
        blocks = [own]
        for k in range(1, outer):
            blocks.append(move(own, lambda o, i: ((o + k) % outer, i)))
        arrived = blocks[1:]
        for k, block in enumerate(blocks):
            arrived += cross(block)
        arrived = [(x,) for x in arrived]
        stages = [[(own,)]]
        stages += [arrived[i : min(i + 3, len(arrived) - 1)] for i in range(0, len(arrived) - 1, 3)]
        stages += [arrived[-1:]] if arrived else []

    share = out_weight.shape[1] // n_tp
    cores = math.gcd(n_tp, 2)
    groups = n_tp // cores
    core, group = tp % cores, tp // cores
    cuts = [0, share // 2, share] if groups == 2 else [0, share]
    widths = [b - a for a, b in zip(cuts, cuts[1:])]
    jobs = [(cut, r) for r in range(1, groups) for cut in range(len(widths))]

    def begins(cut, r):
        to = (group + r) % groups * cores
        firsts = jnp.stack([to + (core + 1) % cores, to + core]) * share
        return (firsts + cuts[cut]).astype(jnp.int32)

    def to_core(x):
        pairs = [(t, t // cores * cores + (t + 1) % cores) for t in range(n_tp)]
        return lax.ppermute(x, "tp", pairs)

    def to_group(x, r):
        pairs = [(t, (t + r * cores) % n_tp) for t in range(n_tp)]
        return lax.ppermute(x, "tp", pairs)

    state = None
    for blocks in stages[:-1]:
        state = attend(block_order, queries, blocks, state, kv_heads)
    cut, r = jobs[0] if jobs else (0, 0)
    attended, send, keep = attend(
        block_order,
        queries,
        stages[-1],
        state,
        kv_heads,
        (begins(cut, r), out_weight, [widths[cut] if jobs else share]),
    )
    arriving = [[] for _ in widths]
    after = ()
    for name, (cut, r) in enumerate(jobs):
        if name > 0:
            send, keep = project(begins(cut, r), attended, out_weight, widths[cut], after)
        if cores > 1:
            keep = keep + to_core(send).astype(jnp.float32)
        total = keep.astype(jnp.bfloat16)
        after = (total,)
        arriving[cut].append(to_group(total, r))
    if jobs:
        send, mine = project(begins(0, 0), attended, out_weight, share, after)
    else:
        mine = keep
    swapped = [to_core(send)] if cores > 1 else []
    return add_up(mine, swapped, arriving, cuts)


def solution(mesh):
    in_specs = (P("ctx", "tp"), P("ctx", None), P("ctx", None), P("tp", None), P("ctx"))
    out_specs = P("ctx", "tp")

    def layer(*args):
        return shards(mesh.shape["ctx"], mesh.shape["tp"], *args)

    return jax.shard_map(
        layer, mesh=mesh, in_specs=in_specs, out_specs=out_specs, check_vma=False
    )
```
